256 devices in a mesh: cohort: 4 (over x, y), tile: 64 (over z, core).
Axes of the slice: x: 2, y: 2, z: 32, core: 2. Of those that a mesh axis runs over, the one named last changes fastest.
The devices are a block of a 4x8x32 slice.
Arguments:
- dosage: bfloat16 [4096, 8192], P(('cohort', 'tile')), parts along dimension 0, may hold values from 0 to 2
- covars: float32 [4096, 16], P(('cohort', 'tile')), parts along dimension 0, may hold values from -12 to 12, as said below
- phenotypes: float32 [4096, 7168], P(('cohort', 'tile')), parts along dimension 0, may hold values from -100 to 100
Outputs:
- mean_chi: float32 [28672], P(('cohort', 'tile')), parts along dimension 0
- hit_rate: float32 [28672], P(('cohort', 'tile')), parts along dimension 0
The draws below stay inside these ranges and needn't reach their ends.
There are 4 independent parts, one for each index of `cohort`. The reference program is written for one: setup_inputs(seed, part) draws one part's arguments, and reference() takes and returns one part's arrays. A program takes and returns all parts, laid end to end along the dimension named above; each array names one. Nothing has to cross between parts.
Inputs may be any that keep to these rules, and one draw needn't show every extreme that they name: `covars`: each covariate column has its own mean and spread.
All inputs are finite; a program needn't handle non-finite values.
Results may differ from the reference program's by a relative error of at most 0.003.
Values may be sent and summed in bfloat16 or wider, within the bound.
A program may use at most 64 MiB of HBM per device.

```python
import math
import jax
import jax.numpy as jnp
from jax import lax

VARIANTS = 8192
COVS = 16
SAMPLES = 1024
GENES = 7168


def ancestry_score(key):
    label = (jax.random.uniform(jax.random.fold_in(key, 14), (SAMPLES,), jnp.float32) < 0.4).astype(jnp.float32)
    blur = jnp.clip(jax.random.normal(jax.random.fold_in(key, 15), (SAMPLES,), jnp.float32), -4.0, 4.0)
    return label + 0.15 * blur


def covar_table(key):
    base = jnp.clip(jax.random.normal(jax.random.fold_in(key, 11), (SAMPLES, COVS), jnp.float32), -5.0, 5.0)
    score = 2.0 * ancestry_score(key) - 1.0
    base = jnp.concatenate([score[:, None], base[:, 1:]], axis=1)
    means = jax.random.uniform(jax.random.fold_in(key, 12), (COVS,), jnp.float32, -2.0, 2.0)
    spread = jnp.exp(jax.random.uniform(jax.random.fold_in(key, 13), (COVS,), jnp.float32, math.log(0.5), math.log(2.0)))
    return base * spread[None, :] + means[None, :]


def draw_covars(key, part):
    return covar_table(key)


def draw_dosage(key, part):
    score = ancestry_score(key)
    base_freq = jax.random.uniform(jax.random.fold_in(key, 31), (VARIANTS,), jnp.float32, 0.05, 0.95)
    shift = jax.random.uniform(jax.random.fold_in(key, 32), (VARIANTS,), jnp.float32, -0.4, 0.4)
    freq = jnp.clip(base_freq[None, :] + shift[None, :] * (score[:, None] - 0.5), 0.02, 0.98)
    first = (jax.random.uniform(jax.random.fold_in(key, 33), (SAMPLES, VARIANTS), jnp.float32) < freq).astype(jnp.float32)
    second = (jax.random.uniform(jax.random.fold_in(key, 34), (SAMPLES, VARIANTS), jnp.float32) < freq).astype(jnp.float32)
    blur = 0.2 * jnp.clip(jax.random.normal(jax.random.fold_in(key, 35), (SAMPLES, VARIANTS), jnp.float32), -3.0, 3.0)
    return jnp.clip(first + second + blur, 0.0, 2.0).astype(jnp.bfloat16)


def draw_phenotypes(key, part):
    table = covar_table(key)
    effect = jnp.clip(jax.random.normal(jax.random.fold_in(key, 21), (COVS, GENES), jnp.float32), -4.0, 4.0)
    spread = jnp.exp(jax.random.uniform(jax.random.fold_in(key, 22), (GENES,), jnp.float32, math.log(0.5), math.log(2.0)))
    noise = jnp.clip(jax.random.normal(jax.random.fold_in(key, 23), (SAMPLES, GENES), jnp.float32), -8.0, 8.0) * spread[None, :]
    signal = jnp.dot(table, effect, precision=lax.Precision.HIGHEST)
    return jnp.clip(signal + noise, -100.0, 100.0)


def setup_inputs(seed: int = 0, part: int = 0) -> dict:
    streams_of = jax.random.split(jax.random.key(seed), 4)
    own_keys = jax.random.split(jax.random.fold_in(streams_of[3], part), 4)
    dosage = draw_dosage(jax.random.fold_in(jax.random.fold_in(streams_of[3], part), 71), part)
    covars = draw_covars(jax.random.fold_in(jax.random.fold_in(streams_of[3], part), 71), part)
    phenotypes = draw_phenotypes(jax.random.fold_in(jax.random.fold_in(streams_of[3], part), 71), part)
    return dict(dosage=dosage, covars=covars, phenotypes=phenotypes)


def reference(dosage, covars, phenotypes):
    highest = lax.Precision.HIGHEST
    dose_real = dosage.astype(jnp.float32)
    samples = dose_real.shape[0]
    variants = dose_real.shape[1]
    gram = jnp.dot(covars.T.astype(jnp.float32), covars.astype(jnp.float32), precision=highest, preferred_element_type=jnp.float32)
    cov_dose = jnp.dot(covars.T.astype(jnp.float32), dose_real.astype(jnp.float32), precision=highest, preferred_element_type=jnp.float32)
    cov_pheno = jnp.dot(covars.T.astype(jnp.float32), phenotypes.astype(jnp.float32), precision=highest, preferred_element_type=jnp.float32)
    factor = jnp.linalg.cholesky(gram)
    betas = jax.scipy.linalg.cho_solve((factor, True), jnp.concatenate([cov_dose, cov_pheno], axis=1))
    beta_dose = betas[:, :variants]
    beta_pheno = betas[:, variants:]
    dose_resid = dose_real - jnp.dot(covars.astype(jnp.float32), beta_dose.astype(jnp.float32), precision=highest, preferred_element_type=jnp.float32)
    pheno_resid = phenotypes - jnp.dot(covars.astype(jnp.float32), beta_pheno.astype(jnp.float32), precision=highest, preferred_element_type=jnp.float32)
    dose_sumsq = lax.optimization_barrier(jnp.sum(dose_resid * dose_resid, axis=0))
    pheno_sumsq = lax.optimization_barrier(jnp.sum(pheno_resid * pheno_resid, axis=0))
    dose_bf = dose_resid.astype(jnp.bfloat16)
    pheno_bf = pheno_resid.astype(jnp.bfloat16)
    cross = lax.dot_general(pheno_bf.astype(jnp.float32), dose_bf.astype(jnp.float32), (((0,), (0,)), ((), ())), preferred_element_type=jnp.float32)
    dose_var = dose_sumsq / samples + 0.1
    pheno_var = pheno_sumsq / samples + 0.1
    zscore = cross / (jnp.sqrt(jnp.float32(samples)) * jnp.sqrt(pheno_var[:, None] * dose_var[None, :]))
    chi_square = zscore * zscore
    mean_chi = lax.optimization_barrier(jnp.mean(chi_square, axis=1))
    hit_rate = 20.0 / variants * lax.optimization_barrier(jnp.sum(jax.nn.sigmoid(2.0 * (chi_square - 4.0)), axis=1))
    return (mean_chi, hit_rate)
```

```python
import functools

import jax
import jax.numpy as jnp
from jax import lax
from jax.experimental import pallas as pl
from jax.experimental.pallas import tpu as pltpu
from jax.sharding import PartitionSpec as P

MESH = pl.DeviceIdType.MESH
LANES = 128
PIECES = 8
FIRST = 4
CW, CCW = 0, 1
F32, BF16 = jnp.float32, jnp.bfloat16


def split3(x):
    hi = x.astype(BF16)
    rest = x - hi.astype(F32)
    mid = rest.astype(BF16)
    lo = (rest - mid.astype(F32)).astype(BF16)
    return hi, mid, lo


def exact_dot(a, b):
    return jnp.dot(a, b, precision=lax.Precision.HIGHEST, preferred_element_type=F32)


def dot(a, b):
    return jnp.dot(a, b, preferred_element_type=F32)


def kernel(
    chips,
    genes,
    dose_ref,
    cov_ref,
    pheno_ref,
    chi_ref,
    hit_ref,
    dose_all,
    cov_all,
    pheno_all,
    stage,
    cw_box,
    ccw_box,
    cov_tile,
    cov_t,
    lhs,
    lhs_fix,
    small,
    gene_scale,
    chi_acc,
    hit_acc,
    mine,
    theirs,
    swap_send,
    swap_recv,
    own_sem,
    ring_send,
    ring_recv,
    ph_send,
    ph_recv,
    cv_send,
    cv_recv,
    pair_send,
    pair_recv,
):
    rows, variants = dose_ref.shape
    covs = cov_ref.shape[1]
    half = variants // 2
    width = half // PIECES
    pad = stage.shape[2]
    samples = rows * 2 * chips
    far = chips // 2
    near = chips - 1 - far

    me = lax.axis_index("tile")
    z, c = me // 2, lax.rem(me, 2)
    other = 1 - c
    partner = 2 * z + other
    right = 2 * lax.rem(z + 1, chips) + c
    left = 2 * lax.rem(z + chips - 1, chips) + c
    towards = (right, left)

    def source(direction, step):
        if direction == CW:
            return lax.rem(z + chips - step, chips)
        return lax.rem(z + step, chips)

    def hops(direction, piece):
        return far if (direction == CW) == (piece % 2 == 0) else near

    barrier = pltpu.get_barrier_semaphore()
    for peer in (partner, right, left):
        pl.semaphore_signal(barrier, inc=1, device_id={"tile": peer}, device_id_type=MESH)
    pl.semaphore_wait(barrier, 3)

    def swap(p):
        cols = pl.ds(pl.multiple_of(other * half + p * width, LANES), width)
        return pltpu.make_async_remote_copy(
            src_ref=dose_ref.at[:, cols],
            dst_ref=dose_all.at[p, z, c],
            send_sem=swap_send.at[p],
            recv_sem=swap_recv.at[p],
            device_id={"tile": partner},
            device_id_type=MESH,
        )

    def own(p):
        cols = pl.ds(pl.multiple_of(c * half + p * width, LANES), width)
        return pltpu.make_async_copy(dose_ref.at[:, cols], dose_all.at[p, z, c], own_sem.at[p])

    def ring(d, p, step, block):
        return pltpu.make_async_remote_copy(
            src_ref=dose_all.at[p, block],
            dst_ref=dose_all.at[p, block],
            send_sem=ring_send.at[d, p, step],
            recv_sem=ring_recv.at[d, p, step],
            device_id={"tile": towards[d]},
            device_id_type=MESH,
        )

    def ring_cov(d, step, block):
        return pltpu.make_async_remote_copy(
            src_ref=cov_all.at[block, c],
            dst_ref=cov_all.at[block, c],
            send_sem=cv_send.at[d, step],
            recv_sem=cv_recv.at[d, step],
            device_id={"tile": towards[d]},
            device_id_type=MESH,
        )

    reach = (far, near)
    boxes = (cw_box, ccw_box)

    def box_start(d, step):
        return sum(reach[d] - k for k in range(step))

    def ring_pheno(d, step):
        count = reach[d] - step
        if step == 0:
            src = stage.at[pl.ds(1, far)] if d == CW else stage.at[pl.ds(far + 1, near)]
        else:
            first = box_start(d, step - 1) + (1 if d == CW else 0)
            src = boxes[d].at[pl.ds(first, count)]
        return pltpu.make_async_remote_copy(
            src_ref=src,
            dst_ref=boxes[d].at[pl.ds(box_start(d, step), count)],
            send_sem=ph_send.at[d, step],
            recv_sem=ph_recv.at[d, step],
            device_id={"tile": towards[d]},
            device_id_type=MESH,
        )

    def keep_pheno(d, step):
        at = box_start(d, step) + (0 if d == CW else reach[d] - step - 1)
        pheno_all[source(d, step + 1), c] = boxes[d][at]

    for p in range(PIECES):
        swap(p).start()
        own(p).start()

    def launch(pieces):
        for p in pieces:
            own(p).wait()
            swap(p).wait_recv()
            for d in (CW, CCW):
                ring(d, p, 0, z).start()

    launch(range(FIRST))

    cov_tile[...] = jnp.zeros_like(cov_tile)
    cov_tile[:, 0:covs] = cov_ref[...]
    hi, mid, lo = split3(cov_tile[...])
    packed = (
        hi.astype(F32)
        + pltpu.roll(mid.astype(F32), covs, 1)
        + pltpu.roll(lo.astype(F32), 2 * covs, 1)
    )
    cov_all[z, c] = packed.astype(BF16)

    for j in range(chips):
        begin = genes * j
        base = begin // LANES * LANES
        wide = min(pad + LANES, pheno_ref.shape[1] - base)
        block = pheno_ref[:, base : base + wide]
        if begin > base:
            block = pltpu.roll(block, wide - (begin - base), 1)
        stage[lax.rem(j - z + chips, chips)] = block[:, :pad]

    for d in (CW, CCW):
        ring_cov(d, 0, z).start()
        ring_pheno(d, 0).start()
    pheno_all[z, c] = stage[0]
    chi_acc[...] = jnp.zeros_like(chi_acc)
    hit_acc[...] = jnp.zeros_like(hit_acc)

    def forward(p, step):
        for d in (CW, CCW):
            if step - 1 < hops(d, p):
                ring(d, p, step - 1, source(d, step)).wait_recv()
            if step < hops(d, p):
                ring(d, p, step, source(d, step)).start()

    for step in range(1, far + 1):
        if step == far:
            launch(range(FIRST, PIECES))
        for d in (CW, CCW):
            if step - 1 < reach[d]:
                ring_cov(d, step - 1, source(d, step)).wait_recv()
            if step < reach[d]:
                ring_cov(d, step, source(d, step)).start()
            if step - 1 < reach[d]:
                ring_pheno(d, step - 1).wait_recv()
            if step < reach[d]:
                ring_pheno(d, step).start()
            if step - 1 < reach[d]:
                keep_pheno(d, step - 1)
        for p in range(FIRST):
            forward(p, step)

    def pair_cov():
        return pltpu.make_async_remote_copy(
            src_ref=cov_all.at[:, c],
            dst_ref=cov_all.at[:, c],
            send_sem=pair_send.at[0],
            recv_sem=pair_recv.at[0],
            device_id={"tile": partner},
            device_id_type=MESH,
        )

    def pair_pheno():
        return pltpu.make_async_remote_copy(
            src_ref=pheno_all.at[:, c],
            dst_ref=pheno_all.at[:, c],
            send_sem=pair_send.at[1],
            recv_sem=pair_recv.at[1],
            device_id={"tile": partner},
            device_id_type=MESH,
        )

    pair_cov().start()
    pair_pheno().start()

    second = range(FIRST, PIECES)

    def forward_all(step):
        for p in second:
            forward(p, step)

    forward_all(1)
    pair_cov().wait_recv()
    cov2 = cov_all[...].reshape(samples, LANES)
    cov_t[...] = jnp.transpose(cov2.astype(F32)).astype(BF16)
    terms = 3 * covs
    lhs[genes : genes + terms] = cov_t[0:terms]
    pairs = dot(cov_t[...], cov2)
    pairs = pairs[0:covs] + pairs[covs : 2 * covs] + pairs[2 * covs : 3 * covs]
    pairs = pairs + pltpu.roll(pairs, LANES - covs, 1) + pltpu.roll(pairs, LANES - 2 * covs, 1)
    lane = lax.broadcasted_iota(jnp.int32, (covs, LANES), 1)
    row = lax.broadcasted_iota(jnp.int32, (covs, LANES), 0)
    gram_wide = jnp.where(lane < covs, pairs, 0.0)
    small[0] = gram_wide

    forward_all(2)

    def eliminate(k, a):
        column = jnp.sum(jnp.where(lane == k, a, 0.0), axis=1, keepdims=True)
        pivot_row = jnp.sum(jnp.where(row == k, a, 0.0), axis=0, keepdims=True)
        pivot = jnp.sum(jnp.where(lane[0:1] == k, pivot_row, 0.0), axis=1, keepdims=True)
        pivot_row = pivot_row / pivot
        return jnp.where(row == k, pivot_row, a - column * pivot_row)

    unit = jnp.where(lane == row + covs, 1.0, 0.0)
    solved = lax.fori_loop(0, covs, eliminate, gram_wide + unit)
    inverse = pltpu.roll(solved, LANES - covs, 1)[:, 0:covs]
    gram = gram_wide[:, 0:covs]
    eye = jnp.where(lane == row, 1.0, 0.0)[:, 0:covs]
    inverse = inverse + exact_dot(inverse, eye - exact_dot(gram, inverse))
    small[1, :, 0:covs] = inverse

    forward_all(3)
    pair_pheno().wait_recv()
    raw = pheno_all[...].reshape(samples, pad)
    cov_pheno = jnp.zeros((terms, pad), F32)
    for part in split3(raw):
        cov_pheno = cov_pheno + dot(cov_t[0:terms], part)
    cov_pheno = cov_pheno[0:covs] + cov_pheno[covs : 2 * covs] + cov_pheno[2 * covs : terms]
    beta = exact_dot(inverse, cov_pheno)
    blank = jnp.zeros((LANES - terms, pad), BF16)
    fit = jnp.zeros((samples, pad), F32)
    cov2 = cov_all[...].reshape(samples, LANES)
    for part in split3(beta):
        fit = fit + dot(cov2, jnp.concatenate([part, part, part, blank], axis=0))
    resid = jnp.transpose(pheno_all[...].reshape(samples, pad) - fit)[0:genes]
    forward_all(4)
    sumsq = jnp.sum(resid * resid, axis=1, keepdims=True)
    scale = 1.0 / (jnp.sqrt(F32(samples)) * jnp.sqrt(sumsq / samples + 0.1))
    gene_scale[...] = jnp.broadcast_to(scale, gene_scale.shape)
    lhs[0:genes] = resid.astype(BF16)
    fix = dot(lhs[0:genes], cov2)
    fix = fix + pltpu.roll(fix, LANES - covs, 1) + pltpu.roll(fix, LANES - 2 * covs, 1)
    fix_lane = lax.broadcasted_iota(jnp.int32, fix.shape, 1)
    lhs_fix[...] = jnp.where(fix_lane < covs, -fix, 0.0).astype(BF16)

    def scan(p):
        dose = dose_all[p].reshape(samples, width)
        both = dot(lhs[...], dose)
        cov_dose = (
            both[genes : genes + covs]
            + both[genes + covs : genes + 2 * covs]
            + both[genes + 2 * covs : genes + 3 * covs]
        )
        beta = exact_dot(small[1, :, 0:covs], cov_dose)
        back = exact_dot(small[0, :, 0:covs], beta)
        real = dose.astype(F32)
        dose_sumsq = jnp.sum(real * real, axis=0, keepdims=True) - jnp.sum(
            beta * (2.0 * cov_dose - back), axis=0, keepdims=True
        )
        dose_scale = 1.0 / jnp.sqrt(dose_sumsq / samples + 0.1)
        blank = jnp.zeros((LANES - covs, width), BF16)
        cross = both[0:genes] + dot(
            lhs_fix[...], jnp.concatenate([beta.astype(BF16), blank], axis=0)
        )
        scale = gene_scale[...]
        chi_sum, hit_sum = chi_acc[0:genes], hit_acc[0:genes]
        for n in range(width // LANES):
            cut = slice(n * LANES, (n + 1) * LANES)
            zscore = cross[:, cut] * dose_scale[:, cut] * scale
            chi = zscore * zscore
            chi_sum = chi_sum + chi
            hit_sum = hit_sum + 1.0 / (1.0 + jnp.exp(8.0 - 2.0 * chi))
        chi_acc[0:genes] = chi_sum
        hit_acc[0:genes] = hit_sum

    todo = list(range(FIRST))
    for step in range(5, far + 1):
        forward_all(step)
        if todo and step % 2 == 1:
            scan(todo.pop(0))
    lax.fori_loop(FIRST - len(todo), PIECES, lambda p, _: (scan(p), 0)[1], 0)

    mine[...] = jnp.zeros_like(mine)
    mine[0:1] = jnp.sum(jnp.transpose(chi_acc[...]), axis=0, keepdims=True)
    mine[1:2] = jnp.sum(jnp.transpose(hit_acc[...]), axis=0, keepdims=True)
    pair = pltpu.make_async_remote_copy(
        src_ref=mine,
        dst_ref=theirs,
        send_sem=pair_send.at[2],
        recv_sem=pair_recv.at[2],
        device_id={"tile": partner},
        device_id_type=MESH,
    )
    pair.start()
    for p in range(PIECES):
        swap(p).wait_send()
        for d in (CW, CCW):
            for step in range(hops(d, p)):
                ring(d, p, step, source(d, step)).wait_send()
    for d in (CW, CCW):
        for step in range(reach[d]):
            ring_cov(d, step, source(d, step)).wait_send()
            ring_pheno(d, step).wait_send()
    pair_cov().wait_send()
    pair_pheno().wait_send()
    pair.wait()
    total = mine[...] + theirs[...]
    own_genes = genes // 2
    total = jnp.where(c == 0, total, pltpu.roll(total, pad - own_genes, 1))
    chi_ref[...] = total[0:1, 0:own_genes] / variants
    hit_ref[...] = 20.0 / variants * total[1:2, 0:own_genes]


def local(dosage, covars, phenotypes):
    devices = lax.axis_size("tile")
    chips = devices // 2
    rows, variants = dosage.shape
    covs = covars.shape[1]
    genes = phenotypes.shape[1] // chips
    pad = -(-genes // LANES) * LANES
    samples = rows * devices
    width = variants // 2 // PIECES
    far = chips // 2
    near = chips - 1 - far
    dma = pltpu.SemaphoreType.DMA
    vmem = pltpu.VMEM
    scratch = [
        vmem((PIECES, chips, 2, rows, width), BF16),
        vmem((chips, 2, rows, LANES), BF16),
        vmem((chips, 2, rows, pad), F32),
        vmem((chips, rows, pad), F32),
        vmem((far * (far + 1) // 2, rows, pad), F32),
        vmem((near * (near + 1) // 2, rows, pad), F32),
        vmem((rows, LANES), F32),
        vmem((LANES, samples), BF16),
        vmem((genes + 3 * covs, samples), BF16),
        vmem((genes, LANES), BF16),
        vmem((2, covs, LANES), F32),
        vmem((genes, LANES), F32),
        vmem((pad, LANES), F32),
        vmem((pad, LANES), F32),
        vmem((8, pad), F32),
        vmem((8, pad), F32),
        dma((PIECES,)),
        dma((PIECES,)),
        dma((PIECES,)),
        dma((2, PIECES, far)),
        dma((2, PIECES, far)),
        dma((2, far)),
        dma((2, far)),
        dma((2, far)),
        dma((2, far)),
        dma((3,)),
        dma((3,)),
    ]
    whole = pl.BlockSpec(memory_space=pltpu.VMEM)
    own_genes = genes // 2
    chi, hit = pl.pallas_call(
        functools.partial(kernel, chips, genes),
        out_shape=[jax.ShapeDtypeStruct((1, own_genes), F32)] * 2,
        in_specs=[whole] * 3,
        out_specs=[whole] * 2,
        scratch_shapes=scratch,
        compiler_params=pltpu.CompilerParams(
            collective_id=0, has_side_effects=True, vmem_limit_bytes=48 * 2**20
        ),
    )(dosage, covars, phenotypes)
    return chi.reshape(own_genes), hit.reshape(own_genes)


def solution(mesh):
    rows = P(("cohort", "tile"), None)
    return jax.shard_map(
        local,
        mesh=mesh,
        in_specs=(rows, rows, rows),
        out_specs=(P(("cohort", "tile")), P(("cohort", "tile"))),
        check_vma=False,
    )
```

```python
import functools

import jax
import jax.numpy as jnp
from jax import lax
from jax.experimental import pallas as pl
from jax.experimental.pallas import tpu as pltpu
from jax.sharding import PartitionSpec as P

MESH = pl.DeviceIdType.MESH
LANES = 128
PIECES = 8
START = (0, 0, 0, 8, 8, 8, 8, 8)
PHENO_TICK = 2
CW, CCW = 0, 1
F32, BF16 = jnp.float32, jnp.bfloat16


def split3(x):
    hi = x.astype(BF16)
    rest = x - hi.astype(F32)
    mid = rest.astype(BF16)
    lo = (rest - mid.astype(F32)).astype(BF16)
    return hi, mid, lo


def exact_dot(a, b):
    return jnp.dot(a, b, precision=lax.Precision.HIGHEST, preferred_element_type=F32)


def dot(a, b):
    return jnp.dot(a, b, preferred_element_type=F32)


def kernel(
    chips,
    genes,
    dose_hbm,
    cov_hbm,
    pheno_hbm,
    chi_ref,
    hit_ref,
    dose_ref,
    cov_ref,
    pheno_ref,
    dose_all,
    cov_all,
    pheno_all,
    stage,
    chip_raw,
    out_box,
    cw_box,
    ccw_box,
    kept,
    cov_tile,
    chip_tile,
    cov_t,
    lhs,
    lhs_fix,
    small,
    gene_scale,
    chi_acc,
    hit_acc,
    mine,
    theirs,
    load_sem,
    swap_send,
    swap_recv,
    own_sem,
    raw_sem,
    ring_send,
    ring_recv,
    ph_send,
    ph_recv,
    cv_send,
    cv_recv,
    pair_send,
    pair_recv,
):
    rows, variants = dose_ref.shape
    covs = cov_ref.shape[1]
    half = variants // 2
    width = half // PIECES
    own_genes = genes // 2
    pad = kept.shape[2]
    samples = rows * 2 * chips
    far = chips // 2
    near = chips - 1 - far

    me = lax.axis_index("tile")
    z, c = me // 2, lax.rem(me, 2)
    other = 1 - c
    partner = 2 * z + other
    right = 2 * lax.rem(z + 1, chips) + c
    left = 2 * lax.rem(z + chips - 1, chips) + c
    towards = (right, left)

    def source(direction, step):
        if direction == CW:
            return lax.rem(z + chips - step, chips)
        return lax.rem(z + step, chips)

    def hops(direction, piece):
        return far if (direction == CW) == (piece == 0) else near

    loads = [
        pltpu.make_async_copy(src, dst, load_sem.at[k])
        for k, (src, dst) in enumerate(
            ((dose_hbm, dose_ref), (cov_hbm, cov_ref), (pheno_hbm, pheno_ref))
        )
    ]
    for copy in loads:
        copy.start()
    barrier = pltpu.get_barrier_semaphore()
    for peer in (partner, right, left):
        pl.semaphore_signal(barrier, inc=1, device_id={"tile": peer}, device_id_type=MESH)
    pl.semaphore_wait(barrier, 3)
    for copy in loads:
        copy.wait()

    def swap(p):
        cols = pl.ds(pl.multiple_of(other * half + p * width, LANES), width)
        return pltpu.make_async_remote_copy(
            src_ref=dose_ref.at[:, cols],
            dst_ref=dose_all.at[p, z, c],
            send_sem=swap_send.at[p],
            recv_sem=swap_recv.at[p],
            device_id={"tile": partner},
            device_id_type=MESH,
        )

    def own(p):
        cols = pl.ds(pl.multiple_of(c * half + p * width, LANES), width)
        return pltpu.make_async_copy(dose_ref.at[:, cols], dose_all.at[p, z, c], own_sem.at[p])

    def ring(d, p, step, block):
        return pltpu.make_async_remote_copy(
            src_ref=dose_all.at[p, block],
            dst_ref=dose_all.at[p, block],
            send_sem=ring_send.at[d, p, step],
            recv_sem=ring_recv.at[d, p, step],
            device_id={"tile": towards[d]},
            device_id_type=MESH,
        )

    def ring_cov(d, step, block):
        return pltpu.make_async_remote_copy(
            src_ref=cov_all.at[block, c],
            dst_ref=cov_all.at[block, c],
            send_sem=cv_send.at[d, step],
            recv_sem=cv_recv.at[d, step],
            device_id={"tile": towards[d]},
            device_id_type=MESH,
        )

    reach = (far, near)
    boxes = (cw_box, ccw_box)

    def box_start(d, step):
        return sum(reach[d] - k for k in range(step))

    def ring_pheno(d, step):
        count = reach[d] - step
        if step == 0:
            src = out_box.at[pl.ds(1, far)] if d == CW else out_box.at[pl.ds(far + 1, near)]
        else:
            first = box_start(d, step - 1) + (1 if d == CW else 0)
            src = boxes[d].at[pl.ds(first, count)]
        return pltpu.make_async_remote_copy(
            src_ref=src,
            dst_ref=boxes[d].at[pl.ds(box_start(d, step), count)],
            send_sem=ph_send.at[d, step],
            recv_sem=ph_recv.at[d, step],
            device_id={"tile": towards[d]},
            device_id_type=MESH,
        )

    def keep_pheno(d, step):
        at = box_start(d, step) + (0 if d == CW else reach[d] - step - 1)
        kept[source(d, step + 1)] = boxes[d][at]

    for p in range(PIECES):
        swap(p).start()
        own(p).start()

    def launch(pieces):
        for p in pieces:
            own(p).wait()
            swap(p).wait_recv()
            for d in (CW, CCW):
                ring(d, p, 0, z).start()

    def tick_of(p):
        return START[p] * far // 16

    launch([p for p in range(PIECES) if tick_of(p) == 0])

    cov_tile[...] = jnp.zeros_like(cov_tile)
    cov_tile[:, 0:covs] = cov_ref[...]
    hi, mid, lo = split3(cov_tile[...])
    packed = (
        hi.astype(F32)
        + pltpu.roll(mid.astype(F32), covs, 1)
        + pltpu.roll(lo.astype(F32), 2 * covs, 1)
    )
    cov_all[z, c] = packed.astype(BF16)
    chip_tile[c] = packed.astype(BF16)

    for j in range(chips):
        place = pl.ds(pl.multiple_of(lax.rem(j - z + chips, chips) * pad, LANES), pad)
        for h in range(2):
            begin = genes * j + own_genes * h
            base = begin // LANES * LANES
            wide = min(pad + LANES, pheno_ref.shape[1] - base)
            block = pheno_ref[:, base : base + wide]
            if begin > base:
                block = pltpu.roll(block, wide - (begin - base), 1)
            stage[h, :, place] = block[:, :pad]

    def pair(slot, src, dst):
        return pltpu.make_async_remote_copy(
            src_ref=src,
            dst_ref=dst,
            send_sem=pair_send.at[slot],
            recv_sem=pair_recv.at[slot],
            device_id={"tile": partner},
            device_id_type=MESH,
        )

    pair_tile = pair(0, chip_tile.at[c], chip_tile.at[c])
    pair_raw = pair(1, stage.at[other], chip_raw.at[c])
    own_raw = pltpu.make_async_copy(stage.at[c], chip_raw.at[c], raw_sem)
    pair_tile.start()
    pair_raw.start()
    own_raw.start()
    for d in (CW, CCW):
        ring_cov(d, 0, z).start()
    chi_acc[...] = jnp.zeros_like(chi_acc)
    hit_acc[...] = jnp.zeros_like(hit_acc)

    lane = lax.broadcasted_iota(jnp.int32, (covs, LANES), 1)
    row = lax.broadcasted_iota(jnp.int32, (covs, LANES), 0)
    terms = 3 * covs

    def three_rows(x):
        return x[0:covs] + x[covs : 2 * covs] + x[2 * covs : terms]

    def three_lanes(x):
        return x + pltpu.roll(x, LANES - covs, 1) + pltpu.roll(x, LANES - 2 * covs, 1)

    def gram_of(x, x_t):
        return jnp.where(lane < covs, three_lanes(three_rows(dot(x_t, x))), 0.0)

    def eliminate(k, a):
        column = jnp.sum(jnp.where(lane == k, a, 0.0), axis=1, keepdims=True)
        pivot_row = jnp.sum(jnp.where(row == k, a, 0.0), axis=0, keepdims=True)
        pivot = jnp.sum(jnp.where(lane[0:1] == k, pivot_row, 0.0), axis=1, keepdims=True)
        pivot_row = pivot_row / pivot
        return jnp.where(row == k, pivot_row, a - column * pivot_row)

    def invert(wide_gram):
        unit = jnp.where(lane == row + covs, 1.0, 0.0)
        solved = lax.fori_loop(0, covs, eliminate, wide_gram + unit)
        return pltpu.roll(solved, LANES - covs, 1)[:, 0:covs]

    def thrice(x):
        blank = jnp.zeros((LANES - terms, x.shape[1]), BF16)
        return jnp.concatenate([x, x, x, blank], axis=0)

    def prepare_pheno():
        pair_tile.wait_recv()
        chip_cov = chip_tile[...].reshape(2 * rows, LANES)
        chip_cov_t = jnp.transpose(chip_cov.astype(F32))
        chip_gram = gram_of(chip_cov, chip_cov_t.astype(BF16))
        ridge = jnp.where(lane == row, chip_gram * 1e-4 + 1e-6, 0.0)
        solve = exact_dot(invert(chip_gram + ridge), three_rows(chip_cov_t))
        solve_hi = solve.astype(BF16)
        solve_lo = (solve - solve_hi.astype(F32)).astype(BF16)
        solver = jnp.concatenate([solve_hi, solve_lo], axis=0)
        own_raw.wait()
        pair_raw.wait_recv()
        group = 8 * pad

        def fit_group(g, carry):
            place = pl.ds(pl.multiple_of(g * group, LANES), group)
            raw = chip_raw[:, :, place].reshape(2 * rows, group)
            both = dot(solver, raw.astype(BF16))
            beta = (both[0:covs] + both[covs : 2 * covs]).astype(BF16)
            left_over = (raw - dot(chip_cov, thrice(beta))).astype(BF16)
            for k in range(8):
                cut = slice(k * pad, (k + 1) * pad)
                out_box[g * 8 + k, 0 : 2 * rows] = left_over[:, cut]
                out_box[g * 8 + k, 2 * rows : 2 * rows + covs] = beta[:, cut]
            return carry

        lax.fori_loop(0, chips // 8, fit_group, 0)

    def launch_pheno():
        for d in (CW, CCW):
            ring_pheno(d, 0).start()
        kept[z] = out_box[0]

    def forward(p, step):
        for d in (CW, CCW):
            if 0 <= step - 1 < hops(d, p):
                ring(d, p, step - 1, source(d, step)).wait_recv()
            if 0 < step < hops(d, p):
                ring(d, p, step, source(d, step)).start()

    sent_at = max(1, PHENO_TICK * far // 16)

    def tick(t):
        launch([p for p in range(PIECES) if t > 0 and tick_of(p) == t])
        for d in (CW, CCW):
            if 0 < t <= reach[d]:
                ring_cov(d, t - 1, source(d, t)).wait_recv()
            if 0 < t < reach[d]:
                ring_cov(d, t, source(d, t)).start()
        step = t - sent_at
        for d in (CW, CCW):
            if 0 < step <= reach[d]:
                ring_pheno(d, step - 1).wait_recv()
            if 0 < step < reach[d]:
                ring_pheno(d, step).start()
            if 0 < step <= reach[d]:
                keep_pheno(d, step - 1)
        for p in sorted(range(PIECES), key=tick_of):
            if 0 < t - tick_of(p) <= far:
                forward(p, t - tick_of(p))

    last = max([tick_of(p) for p in range(PIECES)] + [sent_at + 1]) + far
    pending = list(range(1, last + 1))

    def next_tick():
        if pending:
            tick(pending.pop(0))

    for _ in range(sent_at):
        next_tick()
    prepare_pheno()
    launch_pheno()
    for _ in range(far):
        next_tick()

    pair_cov = pair(2, cov_all.at[:, c], cov_all.at[:, c])
    pair_cov.start()

    next_tick()
    pair_cov.wait_recv()
    cov2 = cov_all[...].reshape(samples, LANES)
    cov_t[...] = jnp.transpose(cov2.astype(F32)).astype(BF16)
    lhs[genes : genes + terms] = cov_t[0:terms]
    gram_wide = gram_of(cov2, cov_t[...])
    small[0] = gram_wide
    inverse = invert(gram_wide)
    eye = jnp.where(lane == row, 1.0, 0.0)[:, 0:covs]
    inverse = inverse + exact_dot(inverse, eye - exact_dot(gram_wide[:, 0:covs], inverse))
    small[1, :, 0:covs] = inverse
    next_tick()

    for k in range(chips):
        block = kept[k]
        fitted = dot(cov_all[k].reshape(2 * rows, LANES), thrice(block[2 * rows :]))
        pheno_all[pl.ds(k * 2 * rows, 2 * rows)] = block[0 : 2 * rows].astype(F32) + fitted
    next_tick()
    cov_pheno = jnp.zeros((terms, pad), F32)
    for part in split3(pheno_all[...]):
        cov_pheno = cov_pheno + dot(cov_t[0:terms], part)
    beta = exact_dot(inverse, three_rows(cov_pheno))
    fit = jnp.zeros((samples, pad), F32)
    cov2 = cov_all[...].reshape(samples, LANES)
    for part in split3(beta):
        fit = fit + dot(cov2, thrice(part))
    resid = jnp.transpose(pheno_all[...] - fit)[0:own_genes]
    sumsq = jnp.sum(resid * resid, axis=1, keepdims=True)
    scale = 1.0 / (jnp.sqrt(F32(samples)) * jnp.sqrt(sumsq / samples + 0.1))
    resid_bf = resid.astype(BF16)
    fix = three_lanes(dot(resid_bf, cov2))
    fix_lane = lax.broadcasted_iota(jnp.int32, fix.shape, 1)
    mine_rows = pl.ds(pl.multiple_of(c * own_genes, 16), own_genes)
    lhs[mine_rows] = resid_bf
    lhs_fix[mine_rows] = jnp.where(fix_lane < covs, -fix, 0.0).astype(BF16)
    gene_scale[mine_rows] = jnp.broadcast_to(scale, (own_genes, LANES))
    next_tick()
    pair_rows = [
        pair(3 + k, ref.at[mine_rows], ref.at[mine_rows])
        for k, ref in enumerate((lhs, lhs_fix, gene_scale))
    ]
    for copy in pair_rows:
        copy.start()
    next_tick()
    for copy in pair_rows:
        copy.wait_recv()

    def scan(p):
        dose = dose_all[p].reshape(samples, width)
        both = dot(lhs[...], dose)
        cov_dose = (
            both[genes : genes + covs]
            + both[genes + covs : genes + 2 * covs]
            + both[genes + 2 * covs : genes + 3 * covs]
        )
        beta = exact_dot(small[1, :, 0:covs], cov_dose)
        back = exact_dot(small[0, :, 0:covs], beta)
        real = dose.astype(F32)
        dose_sumsq = jnp.sum(real * real, axis=0, keepdims=True) - jnp.sum(
            beta * (2.0 * cov_dose - back), axis=0, keepdims=True
        )
        dose_scale = 1.0 / jnp.sqrt(dose_sumsq / samples + 0.1)
        blank = jnp.zeros((LANES - covs, width), BF16)
        cross = both[0:genes] + dot(
            lhs_fix[...], jnp.concatenate([beta.astype(BF16), blank], axis=0)
        )
        scale = gene_scale[...]
        chi_sum, hit_sum = chi_acc[0:genes], hit_acc[0:genes]
        for n in range(width // LANES):
            cut = slice(n * LANES, (n + 1) * LANES)
            zscore = cross[:, cut] * dose_scale[:, cut] * scale
            chi = zscore * zscore
            chi_sum = chi_sum + chi
            hit_sum = hit_sum + 1.0 / (1.0 + jnp.exp(8.0 - 2.0 * chi))
        chi_acc[0:genes] = chi_sum
        hit_acc[0:genes] = hit_sum

    done = 0
    while pending:
        now = pending[0]
        next_tick()
        if done < PIECES and tick_of(done) + far < now:
            scan(done)
            done += 1
    lax.fori_loop(done, PIECES, lambda p, _: (scan(p), 0)[1], 0)

    mine[...] = jnp.zeros_like(mine)
    mine[0:1] = jnp.sum(jnp.transpose(chi_acc[...]), axis=0, keepdims=True)
    mine[1:2] = jnp.sum(jnp.transpose(hit_acc[...]), axis=0, keepdims=True)
    pair_sums = pair(6, mine, theirs)
    pair_sums.start()
    for p in range(PIECES):
        swap(p).wait_send()
        for d in (CW, CCW):
            for step in range(hops(d, p)):
                ring(d, p, step, source(d, step)).wait_send()
    for d in (CW, CCW):
        for step in range(reach[d]):
            ring_cov(d, step, source(d, step)).wait_send()
            ring_pheno(d, step).wait_send()
    for copy in (pair_tile, pair_raw, pair_cov, *pair_rows):
        copy.wait_send()
    pair_sums.wait()
    total = mine[...] + theirs[...]
    total = jnp.where(c == 0, total, pltpu.roll(total, total.shape[1] - own_genes, 1))
    chi_ref[...] = total[0:1, 0:own_genes] / variants
    hit_ref[...] = 20.0 / variants * total[1:2, 0:own_genes]


def local(dosage, covars, phenotypes):
    devices = lax.axis_size("tile")
    chips = devices // 2
    rows, variants = dosage.shape
    covs = covars.shape[1]
    genes = phenotypes.shape[1] // chips
    own_genes = genes // 2
    pad = -(-own_genes // LANES) * LANES
    wide = -(-genes // LANES) * LANES
    sent = 2 * rows + covs
    samples = rows * devices
    width = variants // 2 // PIECES
    far = chips // 2
    near = chips - 1 - far
    dma = pltpu.SemaphoreType.DMA
    vmem = pltpu.VMEM
    scratch = [
        vmem(dosage.shape, BF16),
        vmem(covars.shape, F32),
        vmem(phenotypes.shape, F32),
        vmem((PIECES, chips, 2, rows, width), BF16),
        vmem((chips, 2, rows, LANES), BF16),
        vmem((samples, pad), F32),
        vmem((2, rows, chips * pad), F32),
        vmem((2, rows, chips * pad), F32),
        vmem((chips, sent, pad), BF16),
        vmem((far * (far + 1) // 2, sent, pad), BF16),
        vmem((near * (near + 1) // 2, sent, pad), BF16),
        vmem((chips, sent, pad), BF16),
        vmem((rows, LANES), F32),
        vmem((2, rows, LANES), BF16),
        vmem((LANES, samples), BF16),
        vmem((genes + 3 * covs, samples), BF16),
        vmem((genes, LANES), BF16),
        vmem((2, covs, LANES), F32),
        vmem((genes, LANES), F32),
        vmem((wide, LANES), F32),
        vmem((wide, LANES), F32),
        vmem((8, wide), F32),
        vmem((8, wide), F32),
        dma((3,)),
        dma((PIECES,)),
        dma((PIECES,)),
        dma((PIECES,)),
        dma(()),
        dma((2, PIECES, far)),
        dma((2, PIECES, far)),
        dma((2, far)),
        dma((2, far)),
        dma((2, far)),
        dma((2, far)),
        dma((7,)),
        dma((7,)),
    ]
    whole = pl.BlockSpec(memory_space=pltpu.VMEM)
    chi, hit = pl.pallas_call(
        functools.partial(kernel, chips, genes),
        out_shape=[jax.ShapeDtypeStruct((1, own_genes), F32)] * 2,
        in_specs=[pl.BlockSpec(memory_space=pltpu.HBM)] * 3,
        out_specs=[whole] * 2,
        scratch_shapes=scratch,
        compiler_params=pltpu.CompilerParams(
            collective_id=0, has_side_effects=True, vmem_limit_bytes=48 * 2**20
        ),
    )(dosage, covars, phenotypes)
    return chi.reshape(own_genes), hit.reshape(own_genes)


def solution(mesh):
    rows = P(("cohort", "tile"), None)
    return jax.shard_map(
        local,
        mesh=mesh,
        in_specs=(rows, rows, rows),
        out_specs=(P(("cohort", "tile")), P(("cohort", "tile"))),
        check_vma=False,
    )
```

```python
import functools

import jax
import jax.numpy as jnp
from jax import lax
from jax.experimental import pallas as pl
from jax.experimental.pallas import tpu as pltpu
from jax.sharding import PartitionSpec as P

MESH = pl.DeviceIdType.MESH
LANES = 128
PIECES = 8
START = (0, 0, 0, 9, 9, 9, 9, 9)
PHENO_TICK = 1
CW, CCW = 0, 1
F32, BF16 = jnp.float32, jnp.bfloat16


def split3(x):
    hi = x.astype(BF16)
    rest = x - hi.astype(F32)
    mid = rest.astype(BF16)
    lo = (rest - mid.astype(F32)).astype(BF16)
    return hi, mid, lo


def exact_dot(a, b):
    return jnp.dot(a, b, precision=lax.Precision.HIGHEST, preferred_element_type=F32)


def dot(a, b):
    return jnp.dot(a, b, preferred_element_type=F32)


def kernel(
    chips,
    genes,
    dose_hbm,
    cov_hbm,
    pheno_hbm,
    chi_ref,
    hit_ref,
    dose_ref,
    cov_ref,
    pheno_ref,
    dose_all,
    cov_all,
    pheno_all,
    stage,
    chip_raw,
    out_box,
    cw_box,
    ccw_box,
    kept,
    cov_tile,
    chip_tile,
    cov_t,
    lhs,
    lhs_fix,
    small,
    gene_scale,
    partial,
    partial_sq,
    chi_acc,
    hit_acc,
    mine,
    theirs,
    load_sem,
    swap_send,
    swap_recv,
    own_sem,
    raw_sem,
    ring_send,
    ring_recv,
    ph_send,
    ph_recv,
    cv_send,
    cv_recv,
    pair_send,
    pair_recv,
):
    rows, variants = dose_ref.shape
    covs = cov_ref.shape[1]
    half = variants // 2
    width = half // PIECES
    own_genes = genes // 2
    pad = kept.shape[2]
    samples = rows * 2 * chips
    far = chips // 2
    near = chips - 1 - far

    me = lax.axis_index("tile")
    z, c = me // 2, lax.rem(me, 2)
    other = 1 - c
    partner = 2 * z + other
    right = 2 * lax.rem(z + 1, chips) + c
    left = 2 * lax.rem(z + chips - 1, chips) + c
    towards = (right, left)

    def slot(direction, step):
        return (chips - step) % chips if direction == CW else step

    def hops(direction, piece):
        return far if (direction == CW) == (piece == 0) else near

    loads = [
        pltpu.make_async_copy(src, dst, load_sem.at[k])
        for k, (src, dst) in enumerate(
            ((dose_hbm, dose_ref), (cov_hbm, cov_ref), (pheno_hbm, pheno_ref))
        )
    ]
    for copy in loads:
        copy.start()
    barrier = pltpu.get_barrier_semaphore()
    for peer in (partner, right, left):
        pl.semaphore_signal(barrier, inc=1, device_id={"tile": peer}, device_id_type=MESH)
    pl.semaphore_wait(barrier, 3)
    for copy in loads:
        copy.wait()

    def swap(p):
        cols = pl.ds(pl.multiple_of(other * half + p * width, LANES), width)
        return pltpu.make_async_remote_copy(
            src_ref=dose_ref.at[:, cols],
            dst_ref=dose_all.at[p, 0, c],
            send_sem=swap_send.at[p],
            recv_sem=swap_recv.at[p],
            device_id={"tile": partner},
            device_id_type=MESH,
        )

    def own(p):
        cols = pl.ds(pl.multiple_of(c * half + p * width, LANES), width)
        return pltpu.make_async_copy(dose_ref.at[:, cols], dose_all.at[p, 0, c], own_sem.at[p])

    def ring(d, p, step):
        return pltpu.make_async_remote_copy(
            src_ref=dose_all.at[p, slot(d, step)],
            dst_ref=dose_all.at[p, slot(d, step + 1)],
            send_sem=ring_send.at[d, p, step],
            recv_sem=ring_recv.at[d, p, step],
            device_id={"tile": towards[d]},
            device_id_type=MESH,
        )

    def ring_cov(d, step):
        return pltpu.make_async_remote_copy(
            src_ref=cov_all.at[slot(d, step), c],
            dst_ref=cov_all.at[slot(d, step + 1), c],
            send_sem=cv_send.at[d, step],
            recv_sem=cv_recv.at[d, step],
            device_id={"tile": towards[d]},
            device_id_type=MESH,
        )

    reach = (far, near)
    boxes = (cw_box, ccw_box)

    def box_start(d, step):
        return sum(reach[d] - k for k in range(step))

    def ring_pheno(d, step):
        count = reach[d] - step
        if step == 0:
            src = out_box.at[pl.ds(1, far)] if d == CW else out_box.at[pl.ds(far + 1, near)]
        else:
            first = box_start(d, step - 1) + (1 if d == CW else 0)
            src = boxes[d].at[pl.ds(first, count)]
        return pltpu.make_async_remote_copy(
            src_ref=src,
            dst_ref=boxes[d].at[pl.ds(box_start(d, step), count)],
            send_sem=ph_send.at[d, step],
            recv_sem=ph_recv.at[d, step],
            device_id={"tile": towards[d]},
            device_id_type=MESH,
        )

    def keep_pheno(d, step):
        at = box_start(d, step) + (0 if d == CW else reach[d] - step - 1)
        kept[slot(d, step + 1)] = boxes[d][at]

    for p in range(PIECES):
        swap(p).start()
        own(p).start()

    def launch(pieces):
        for p in pieces:
            own(p).wait()
            swap(p).wait_recv()
            for d in (CW, CCW):
                ring(d, p, 0).start()

    def tick_of(p):
        return START[p] * far // 16

    launch([p for p in range(PIECES) if tick_of(p) == 0])

    cov_tile[...] = jnp.zeros_like(cov_tile)
    cov_tile[:, 0:covs] = cov_ref[...]
    hi, mid, lo = split3(cov_tile[...])
    packed = (
        hi.astype(F32)
        + pltpu.roll(mid.astype(F32), covs, 1)
        + pltpu.roll(lo.astype(F32), 2 * covs, 1)
    )
    cov_all[0, c] = packed.astype(BF16)
    chip_tile[c] = packed.astype(BF16)

    for j in range(chips):
        place = pl.ds(pl.multiple_of(lax.rem(j - z + chips, chips) * pad, LANES), pad)
        for h in range(2):
            begin = genes * j + own_genes * h
            base = begin // LANES * LANES
            wide = min(pad + LANES, pheno_ref.shape[1] - base)
            block = pheno_ref[:, base : base + wide]
            if begin > base:
                block = pltpu.roll(block, wide - (begin - base), 1)
            stage[h, :, place] = block[:, :pad]

    def pair(slot, src, dst):
        return pltpu.make_async_remote_copy(
            src_ref=src,
            dst_ref=dst,
            send_sem=pair_send.at[slot],
            recv_sem=pair_recv.at[slot],
            device_id={"tile": partner},
            device_id_type=MESH,
        )

    pair_tile = pair(0, chip_tile.at[c], chip_tile.at[c])
    pair_raw = pair(1, stage.at[other], chip_raw.at[c])
    own_raw = pltpu.make_async_copy(stage.at[c], chip_raw.at[c], raw_sem)
    pair_tile.start()
    pair_raw.start()
    own_raw.start()
    for d in (CW, CCW):
        ring_cov(d, 0).start()
    chi_acc[...] = jnp.zeros_like(chi_acc)
    hit_acc[...] = jnp.zeros_like(hit_acc)

    lane = lax.broadcasted_iota(jnp.int32, (covs, LANES), 1)
    row = lax.broadcasted_iota(jnp.int32, (covs, LANES), 0)
    terms = 3 * covs

    def three_rows(x):
        return x[0:covs] + x[covs : 2 * covs] + x[2 * covs : terms]

    def three_lanes(x):
        return x + pltpu.roll(x, LANES - covs, 1) + pltpu.roll(x, LANES - 2 * covs, 1)

    def gram_of(x, x_t):
        return jnp.where(lane < covs, three_lanes(three_rows(dot(x_t, x))), 0.0)

    def eliminate(k, a):
        column = jnp.sum(jnp.where(lane == k, a, 0.0), axis=1, keepdims=True)
        pivot_row = jnp.sum(jnp.where(row == k, a, 0.0), axis=0, keepdims=True)
        pivot = jnp.sum(jnp.where(lane[0:1] == k, pivot_row, 0.0), axis=1, keepdims=True)
        pivot_row = pivot_row / pivot
        return jnp.where(row == k, pivot_row, a - column * pivot_row)

    def invert(wide_gram):
        unit = jnp.where(lane == row + covs, 1.0, 0.0)
        solved = lax.fori_loop(0, covs, eliminate, wide_gram + unit)
        return pltpu.roll(solved, LANES - covs, 1)[:, 0:covs]

    def thrice(x):
        blank = jnp.zeros((LANES - terms, x.shape[1]), BF16)
        return jnp.concatenate([x, x, x, blank], axis=0)

    def prepare_pheno():
        pair_tile.wait_recv()
        chip_cov = chip_tile[...].reshape(2 * rows, LANES)
        chip_cov_t = jnp.transpose(chip_cov.astype(F32))
        chip_gram = gram_of(chip_cov, chip_cov_t.astype(BF16))
        ridge = jnp.where(lane == row, chip_gram * 1e-4 + 1e-6, 0.0)
        solve = exact_dot(invert(chip_gram + ridge), three_rows(chip_cov_t))
        solve_hi = solve.astype(BF16)
        solve_lo = (solve - solve_hi.astype(F32)).astype(BF16)
        solver = jnp.concatenate([solve_hi, solve_lo], axis=0)
        next_tick()
        own_raw.wait()
        pair_raw.wait_recv()
        group = 8 * pad

        def fit_group(g, carry):
            place = pl.ds(pl.multiple_of(g * group, LANES), group)
            raw = chip_raw[:, :, place].reshape(2 * rows, group)
            both = dot(solver, raw.astype(BF16))
            beta = (both[0:covs] + both[covs : 2 * covs]).astype(BF16)
            left_over = (raw - dot(chip_cov, thrice(beta))).astype(BF16)
            for k in range(8):
                cut = slice(k * pad, (k + 1) * pad)
                out_box[g * 8 + k, 0 : 2 * rows] = left_over[:, cut]
                out_box[g * 8 + k, 2 * rows : 2 * rows + covs] = beta[:, cut]
            return carry

        half_groups = chips // 16
        lax.fori_loop(0, half_groups, fit_group, 0)
        next_tick()
        lax.fori_loop(half_groups, chips // 8, fit_group, 0)

    def launch_pheno():
        for d in (CW, CCW):
            ring_pheno(d, 0).start()
        kept[0] = out_box[0]

    def forward(p, step):
        for d in (CW, CCW):
            if 0 <= step - 1 < hops(d, p):
                ring(d, p, step - 1).wait_recv()
            if 0 < step < hops(d, p):
                ring(d, p, step).start()

    sent_at = 2 + PHENO_TICK

    def tick(t):
        launch([p for p in range(PIECES) if t > 0 and tick_of(p) == t])
        for d in (CW, CCW):
            if 0 < t <= reach[d]:
                ring_cov(d, t - 1).wait_recv()
            if 0 < t < reach[d]:
                ring_cov(d, t).start()
        step = t - sent_at
        for d in (CW, CCW):
            if 0 < step <= reach[d]:
                ring_pheno(d, step - 1).wait_recv()
            if 0 < step < reach[d]:
                ring_pheno(d, step).start()
            if 0 < step <= reach[d]:
                keep_pheno(d, step - 1)
        for p in sorted(range(PIECES), key=tick_of):
            if 0 < t - tick_of(p) <= far:
                forward(p, t - tick_of(p))

    last = max([tick_of(p) for p in range(PIECES)] + [sent_at + 1]) + far
    pending = list(range(1, last + 1))

    def now():
        return pending[0] if pending else last + 1

    def next_tick():
        if pending:
            tick(pending.pop(0))

    for _ in range(sent_at - 2):
        next_tick()
    prepare_pheno()
    launch_pheno()
    while now() <= far:
        next_tick()

    pair_cov = pair(2, cov_all.at[:, c], cov_all.at[:, c])
    pair_cov.start()

    next_tick()
    pair_cov.wait_recv()
    cov2 = cov_all[...].reshape(samples, LANES)
    cov_t[...] = jnp.transpose(cov2.astype(F32)).astype(BF16)
    lhs[genes : genes + terms] = cov_t[0:terms]
    gram_wide = gram_of(cov2, cov_t[...])
    small[0] = gram_wide
    inverse = invert(gram_wide)
    eye = jnp.where(lane == row, 1.0, 0.0)[:, 0:covs]
    inverse = inverse + exact_dot(inverse, eye - exact_dot(gram_wide[:, 0:covs], inverse))
    small[1, :, 0:covs] = inverse
    while now() <= min(last, sent_at + far):
        next_tick()

    for k in range(chips):
        block = kept[k]
        fitted = dot(cov_all[k].reshape(2 * rows, LANES), thrice(block[2 * rows :]))
        pheno_all[pl.ds(k * 2 * rows, 2 * rows)] = block[0 : 2 * rows].astype(F32) + fitted
    cov_pheno = jnp.zeros((terms, pad), F32)
    for part in split3(pheno_all[...]):
        cov_pheno = cov_pheno + dot(cov_t[0:terms], part)
    beta = exact_dot(inverse, three_rows(cov_pheno))
    fit = jnp.zeros((samples, pad), F32)
    cov2 = cov_all[...].reshape(samples, LANES)
    for part in split3(beta):
        fit = fit + dot(cov2, thrice(part))
    resid = jnp.transpose(pheno_all[...] - fit)[0:own_genes]
    sumsq = jnp.sum(resid * resid, axis=1, keepdims=True)
    scale = 1.0 / (jnp.sqrt(F32(samples)) * jnp.sqrt(sumsq / samples + 0.1))
    resid_bf = resid.astype(BF16)
    fix = three_lanes(dot(resid_bf, cov2))
    fix_lane = lax.broadcasted_iota(jnp.int32, fix.shape, 1)
    mine_rows = pl.ds(pl.multiple_of(c * own_genes, 16), own_genes)
    lhs[mine_rows] = resid_bf
    lhs_fix[mine_rows] = jnp.where(fix_lane < covs, -fix, 0.0).astype(BF16)
    gene_scale[mine_rows] = jnp.broadcast_to(scale, (own_genes, LANES))
    next_tick()
    pair_rows = [
        pair(3 + k, ref.at[mine_rows], ref.at[mine_rows])
        for k, ref in enumerate((lhs, lhs_fix, gene_scale))
    ]
    for copy in pair_rows:
        copy.start()
    next_tick()
    for copy in pair_rows:
        copy.wait_recv()

    cut = far * 3 // 4 // 4 * 4
    low, high = cut * 2 * rows, (chips - cut) * 2 * rows

    def part(first, final, p):
        dose = dose_all[p, first:final].reshape((final - first) * 2 * rows, width)
        real = dose.astype(F32)
        return (
            dot(lhs[:, first * 2 * rows : final * 2 * rows], dose),
            jnp.sum(real * real, axis=0, keepdims=True),
        )

    def near_part(p):
        if cut:
            before, after = part(0, cut, p), part(chips - cut, chips, p)
            partial[p] = before[0] + after[0]
            partial_sq[p, 0:1] = before[1] + after[1]
        else:
            partial[p] = jnp.zeros(partial.shape[1:], F32)
            partial_sq[p] = jnp.zeros(partial_sq.shape[1:], F32)

    def finish(p):
        both, dose_sq = part(cut, chips - cut, p)
        both = both + partial[p]
        dose_sq = dose_sq + partial_sq[p, 0:1]
        cov_dose = three_rows(both[genes:])
        beta = exact_dot(small[1, :, 0:covs], cov_dose)
        back = exact_dot(small[0, :, 0:covs], beta)
        dose_sumsq = dose_sq - jnp.sum(beta * (2.0 * cov_dose - back), axis=0, keepdims=True)
        dose_scale = 1.0 / jnp.sqrt(dose_sumsq / samples + 0.1)
        blank = jnp.zeros((LANES - covs, width), BF16)
        cross = both[0:genes] + dot(
            lhs_fix[...], jnp.concatenate([beta.astype(BF16), blank], axis=0)
        )
        scale = gene_scale[...]
        chi_sum, hit_sum = chi_acc[0:genes], hit_acc[0:genes]
        for n in range(width // LANES):
            span = slice(n * LANES, (n + 1) * LANES)
            zscore = cross[:, span] * dose_scale[:, span] * scale
            chi = zscore * zscore
            chi_sum = chi_sum + chi
            hit_sum = hit_sum + 1.0 / (1.0 + jnp.exp(8.0 - 2.0 * chi))
        chi_acc[0:genes] = chi_sum
        hit_acc[0:genes] = hit_sum

    def over(work, begin, end):
        lax.fori_loop(begin, end, lambda p, _: (work(p), 0)[1], 0)

    early = sum(tick_of(p) + far < now() for p in range(PIECES))
    over(near_part, 0, early)
    next_tick()
    over(finish, 0, early)
    next_tick()
    while pending and now() <= last - far // 4 + 1:
        next_tick()
    over(near_part, early, PIECES)
    while pending:
        next_tick()
    over(finish, early, PIECES)

    mine[...] = jnp.zeros_like(mine)
    mine[0:1] = jnp.sum(jnp.transpose(chi_acc[...]), axis=0, keepdims=True)
    mine[1:2] = jnp.sum(jnp.transpose(hit_acc[...]), axis=0, keepdims=True)
    pair_sums = pair(6, mine, theirs)
    pair_sums.start()
    for p in range(PIECES):
        swap(p).wait_send()
        for d in (CW, CCW):
            for step in range(hops(d, p)):
                ring(d, p, step).wait_send()
    for d in (CW, CCW):
        for step in range(reach[d]):
            ring_cov(d, step).wait_send()
            ring_pheno(d, step).wait_send()
    for copy in (pair_tile, pair_raw, pair_cov, *pair_rows):
        copy.wait_send()
    pair_sums.wait()
    total = mine[...] + theirs[...]
    total = jnp.where(c == 0, total, pltpu.roll(total, total.shape[1] - own_genes, 1))
    chi_ref[...] = total[0:1, 0:own_genes] / variants
    hit_ref[...] = 20.0 / variants * total[1:2, 0:own_genes]


def local(dosage, covars, phenotypes):
    devices = lax.axis_size("tile")
    chips = devices // 2
    rows, variants = dosage.shape
    covs = covars.shape[1]
    genes = phenotypes.shape[1] // chips
    own_genes = genes // 2
    pad = -(-own_genes // LANES) * LANES
    wide = -(-genes // LANES) * LANES
    sent = 2 * rows + covs
    samples = rows * devices
    width = variants // 2 // PIECES
    far = chips // 2
    near = chips - 1 - far
    dma = pltpu.SemaphoreType.DMA
    vmem = pltpu.VMEM
    scratch = [
        vmem(dosage.shape, BF16),
        vmem(covars.shape, F32),
        vmem(phenotypes.shape, F32),
        vmem((PIECES, chips, 2, rows, width), BF16),
        vmem((chips, 2, rows, LANES), BF16),
        vmem((samples, pad), F32),
        vmem((2, rows, chips * pad), F32),
        vmem((2, rows, chips * pad), F32),
        vmem((chips, sent, pad), BF16),
        vmem((far * (far + 1) // 2, sent, pad), BF16),
        vmem((near * (near + 1) // 2, sent, pad), BF16),
        vmem((chips, sent, pad), BF16),
        vmem((rows, LANES), F32),
        vmem((2, rows, LANES), BF16),
        vmem((LANES, samples), BF16),
        vmem((genes + 3 * covs, samples), BF16),
        vmem((genes, LANES), BF16),
        vmem((2, covs, LANES), F32),
        vmem((genes, LANES), F32),
        vmem((PIECES, genes + 3 * covs, width), F32),
        vmem((PIECES, 8, width), F32),
        vmem((wide, LANES), F32),
        vmem((wide, LANES), F32),
        vmem((8, wide), F32),
        vmem((8, wide), F32),
        dma((3,)),
        dma((PIECES,)),
        dma((PIECES,)),
        dma((PIECES,)),
        dma(()),
        dma((2, PIECES, far)),
        dma((2, PIECES, far)),
        dma((2, far)),
        dma((2, far)),
        dma((2, far)),
        dma((2, far)),
        dma((7,)),
        dma((7,)),
    ]
    whole = pl.BlockSpec(memory_space=pltpu.VMEM)
    chi, hit = pl.pallas_call(
        functools.partial(kernel, chips, genes),
        out_shape=[jax.ShapeDtypeStruct((1, own_genes), F32)] * 2,
        in_specs=[pl.BlockSpec(memory_space=pltpu.HBM)] * 3,
        out_specs=[whole] * 2,
        scratch_shapes=scratch,
        compiler_params=pltpu.CompilerParams(
            collective_id=0, has_side_effects=True, vmem_limit_bytes=48 * 2**20
        ),
    )(dosage, covars, phenotypes)
    return chi.reshape(own_genes), hit.reshape(own_genes)


def solution(mesh):
    rows = P(("cohort", "tile"), None)
    return jax.shard_map(
        local,
        mesh=mesh,
        in_specs=(rows, rows, rows),
        out_specs=(P(("cohort", "tile")), P(("cohort", "tile"))),
        check_vma=False,
    )
```

```python
import functools

import jax
import jax.numpy as jnp
from jax import lax
from jax.experimental import pallas as pl
from jax.experimental.pallas import tpu as pltpu
from jax.sharding import PartitionSpec as P

MESH = pl.DeviceIdType.MESH
LANES = 128
PIECES = 8
START = (0, 0, 0, 9, 9, 9, 9, 9)
PHENO_TICK = 1
CW, CCW = 0, 1
F32, BF16 = jnp.float32, jnp.bfloat16


def split3(x):
    hi = x.astype(BF16)
    rest = x - hi.astype(F32)
    mid = rest.astype(BF16)
    lo = (rest - mid.astype(F32)).astype(BF16)
    return hi, mid, lo


def exact_dot(a, b):
    return jnp.dot(a, b, precision=lax.Precision.HIGHEST, preferred_element_type=F32)


def dot(a, b):
    return jnp.dot(a, b, preferred_element_type=F32)


def kernel(
    chips,
    genes,
    dose_hbm,
    cov_hbm,
    pheno_hbm,
    chi_ref,
    hit_ref,
    dose_ref,
    cov_ref,
    pheno_ref,
    dose_all,
    cov_all,
    pheno_all,
    stage,
    chip_raw,
    out_box,
    cw_box,
    ccw_box,
    kept,
    cov_tile,
    chip_tile,
    cov_t,
    lhs,
    lhs_fix,
    small,
    gene_scale,
    partial,
    partial_sq,
    cov_dose_all,
    dose_sq_all,
    beta_all,
    chi_acc,
    hit_acc,
    mine,
    theirs,
    load_sem,
    swap_send,
    swap_recv,
    own_sem,
    raw_sem,
    ring_send,
    ring_recv,
    ph_send,
    ph_recv,
    cv_send,
    cv_recv,
    pair_send,
    pair_recv,
):
    rows, variants = dose_ref.shape
    covs = cov_ref.shape[1]
    half = variants // 2
    width = half // PIECES
    own_genes = genes // 2
    pad = kept.shape[2]
    samples = rows * 2 * chips
    far = chips // 2
    near = chips - 1 - far

    me = lax.axis_index("tile")
    z, c = me // 2, lax.rem(me, 2)
    other = 1 - c
    partner = 2 * z + other
    right = 2 * lax.rem(z + 1, chips) + c
    left = 2 * lax.rem(z + chips - 1, chips) + c
    towards = (right, left)

    def slot(direction, step):
        return (chips - step) % chips if direction == CW else step

    def hops(direction, piece):
        return far if (direction == CW) == (piece == 0) else near

    loads = [
        pltpu.make_async_copy(src, dst, load_sem.at[k])
        for k, (src, dst) in enumerate(
            ((dose_hbm, dose_ref), (cov_hbm, cov_ref), (pheno_hbm, pheno_ref))
        )
    ]
    for copy in loads:
        copy.start()
    barrier = pltpu.get_barrier_semaphore()
    for peer in (partner, right, left):
        pl.semaphore_signal(barrier, inc=1, device_id={"tile": peer}, device_id_type=MESH)
    pl.semaphore_wait(barrier, 3)
    loads[0].wait()

    def swap(p):
        cols = pl.ds(pl.multiple_of(other * half + p * width, LANES), width)
        return pltpu.make_async_remote_copy(
            src_ref=dose_ref.at[:, cols],
            dst_ref=dose_all.at[p, 0, c],
            send_sem=swap_send.at[p],
            recv_sem=swap_recv.at[p],
            device_id={"tile": partner},
            device_id_type=MESH,
        )

    def own(p):
        cols = pl.ds(pl.multiple_of(c * half + p * width, LANES), width)
        return pltpu.make_async_copy(dose_ref.at[:, cols], dose_all.at[p, 0, c], own_sem.at[p])

    def ring(d, p, step):
        return pltpu.make_async_remote_copy(
            src_ref=dose_all.at[p, slot(d, step)],
            dst_ref=dose_all.at[p, slot(d, step + 1)],
            send_sem=ring_send.at[d, p, step],
            recv_sem=ring_recv.at[d, p, step],
            device_id={"tile": towards[d]},
            device_id_type=MESH,
        )

    def ring_cov(d, step):
        return pltpu.make_async_remote_copy(
            src_ref=cov_all.at[slot(d, step), c],
            dst_ref=cov_all.at[slot(d, step + 1), c],
            send_sem=cv_send.at[d, step],
            recv_sem=cv_recv.at[d, step],
            device_id={"tile": towards[d]},
            device_id_type=MESH,
        )

    reach = (far, near)
    boxes = (cw_box, ccw_box)

    def box_start(d, step):
        return sum(reach[d] - k for k in range(step))

    def ring_pheno(d, step):
        count = reach[d] - step
        if step == 0:
            src = out_box.at[pl.ds(1, far)] if d == CW else out_box.at[pl.ds(far + 1, near)]
        else:
            first = box_start(d, step - 1) + (1 if d == CW else 0)
            src = boxes[d].at[pl.ds(first, count)]
        return pltpu.make_async_remote_copy(
            src_ref=src,
            dst_ref=boxes[d].at[pl.ds(box_start(d, step), count)],
            send_sem=ph_send.at[d, step],
            recv_sem=ph_recv.at[d, step],
            device_id={"tile": towards[d]},
            device_id_type=MESH,
        )

    def keep_pheno(d, step):
        at = box_start(d, step) + (0 if d == CW else reach[d] - step - 1)
        kept[slot(d, step + 1)] = boxes[d][at]

    for p in range(PIECES):
        swap(p).start()
        own(p).start()

    def launch(pieces):
        for p in pieces:
            own(p).wait()
            swap(p).wait_recv()
            for d in (CW, CCW):
                ring(d, p, 0).start()

    def tick_of(p):
        return START[p] * far // 16

    launch([p for p in range(PIECES) if tick_of(p) == 0])

    loads[1].wait()
    cov_tile[...] = jnp.zeros_like(cov_tile)
    cov_tile[:, 0:covs] = cov_ref[...]
    hi, mid, lo = split3(cov_tile[...])
    packed = (
        hi.astype(F32)
        + pltpu.roll(mid.astype(F32), covs, 1)
        + pltpu.roll(lo.astype(F32), 2 * covs, 1)
    )
    cov_all[0, c] = packed.astype(BF16)
    chip_tile[c] = packed.astype(BF16)

    loads[2].wait()
    for j in range(chips):
        place = pl.ds(pl.multiple_of(lax.rem(j - z + chips, chips) * pad, LANES), pad)
        for h in range(2):
            begin = genes * j + own_genes * h
            base = begin // LANES * LANES
            wide = min(pad + LANES, pheno_ref.shape[1] - base)
            block = pheno_ref[:, base : base + wide]
            if begin > base:
                block = pltpu.roll(block, wide - (begin - base), 1)
            stage[h, :, place] = block[:, :pad]

    def pair(slot, src, dst):
        return pltpu.make_async_remote_copy(
            src_ref=src,
            dst_ref=dst,
            send_sem=pair_send.at[slot],
            recv_sem=pair_recv.at[slot],
            device_id={"tile": partner},
            device_id_type=MESH,
        )

    pair_tile = pair(0, chip_tile.at[c], chip_tile.at[c])
    pair_raw = pair(1, stage.at[other], chip_raw.at[c])
    own_raw = pltpu.make_async_copy(stage.at[c], chip_raw.at[c], raw_sem)
    pair_tile.start()
    pair_raw.start()
    own_raw.start()
    for d in (CW, CCW):
        ring_cov(d, 0).start()
    chi_acc[...] = jnp.zeros_like(chi_acc)
    hit_acc[...] = jnp.zeros_like(hit_acc)

    lane = lax.broadcasted_iota(jnp.int32, (covs, LANES), 1)
    row = lax.broadcasted_iota(jnp.int32, (covs, LANES), 0)
    terms = 3 * covs

    def three_rows(x):
        return x[0:covs] + x[covs : 2 * covs] + x[2 * covs : terms]

    def three_lanes(x):
        return x + pltpu.roll(x, LANES - covs, 1) + pltpu.roll(x, LANES - 2 * covs, 1)

    def gram_of(x, x_t):
        return jnp.where(lane < covs, three_lanes(three_rows(dot(x_t, x))), 0.0)

    def eliminate(k, a):
        column = jnp.sum(jnp.where(lane == k, a, 0.0), axis=1, keepdims=True)
        pivot_row = jnp.sum(jnp.where(row == k, a, 0.0), axis=0, keepdims=True)
        pivot = jnp.sum(jnp.where(lane[0:1] == k, pivot_row, 0.0), axis=1, keepdims=True)
        pivot_row = pivot_row / pivot
        return jnp.where(row == k, pivot_row, a - column * pivot_row)

    def invert(wide_gram):
        unit = jnp.where(lane == row + covs, 1.0, 0.0)
        solved = lax.fori_loop(0, covs, eliminate, wide_gram + unit)
        return pltpu.roll(solved, LANES - covs, 1)[:, 0:covs]

    def thrice(x):
        blank = jnp.zeros((LANES - terms, x.shape[1]), BF16)
        return jnp.concatenate([x, x, x, blank], axis=0)

    def prepare_pheno():
        pair_tile.wait_recv()
        chip_cov = chip_tile[...].reshape(2 * rows, LANES)
        chip_cov_t = jnp.transpose(chip_cov.astype(F32))
        chip_gram = gram_of(chip_cov, chip_cov_t.astype(BF16))
        ridge = jnp.where(lane == row, chip_gram * 1e-4 + 1e-6, 0.0)
        solve = exact_dot(invert(chip_gram + ridge), three_rows(chip_cov_t))
        solve_hi = solve.astype(BF16)
        solve_lo = (solve - solve_hi.astype(F32)).astype(BF16)
        solver = jnp.concatenate([solve_hi, solve_lo], axis=0)
        next_tick()
        own_raw.wait()
        pair_raw.wait_recv()
        group = 8 * pad

        def fit_group(g, carry):
            place = pl.ds(pl.multiple_of(g * group, LANES), group)
            raw = chip_raw[:, :, place].reshape(2 * rows, group)
            both = dot(solver, raw.astype(BF16))
            beta = (both[0:covs] + both[covs : 2 * covs]).astype(BF16)
            left_over = (raw - dot(chip_cov, thrice(beta))).astype(BF16)
            for k in range(8):
                cut = slice(k * pad, (k + 1) * pad)
                out_box[g * 8 + k, 0 : 2 * rows] = left_over[:, cut]
                out_box[g * 8 + k, 2 * rows : 2 * rows + covs] = beta[:, cut]
            return carry

        half_groups = chips // 16
        lax.fori_loop(0, half_groups, fit_group, 0)
        next_tick()
        lax.fori_loop(half_groups, chips // 8, fit_group, 0)

    def launch_pheno():
        for d in (CW, CCW):
            ring_pheno(d, 0).start()
        kept[0] = out_box[0]

    def forward(p, step):
        for d in (CW, CCW):
            if 0 <= step - 1 < hops(d, p):
                ring(d, p, step - 1).wait_recv()
            if 0 < step < hops(d, p):
                ring(d, p, step).start()

    sent_at = 2 + PHENO_TICK

    def tick(t):
        launch([p for p in range(PIECES) if t > 0 and tick_of(p) == t])
        for d in (CW, CCW):
            if 0 < t <= reach[d]:
                ring_cov(d, t - 1).wait_recv()
            if 0 < t < reach[d]:
                ring_cov(d, t).start()
        for p in sorted(range(PIECES), key=tick_of):
            if 0 < t - tick_of(p) <= far:
                forward(p, t - tick_of(p))
        step = t - sent_at
        for d in (CW, CCW):
            if 0 < step <= reach[d]:
                ring_pheno(d, step - 1).wait_recv()
            if 0 < step < reach[d]:
                ring_pheno(d, step).start()
            if 0 < step <= reach[d]:
                keep_pheno(d, step - 1)

    last = max([tick_of(p) for p in range(PIECES)] + [sent_at + 1]) + far
    pending = list(range(1, last + 1))

    def now():
        return pending[0] if pending else last + 1

    def next_tick():
        if pending:
            tick(pending.pop(0))

    for _ in range(sent_at - 2):
        next_tick()
    prepare_pheno()
    launch_pheno()
    while now() <= far:
        next_tick()

    pair_cov = pair(2, cov_all.at[:, c], cov_all.at[:, c])
    pair_cov.start()

    next_tick()
    pair_cov.wait_recv()
    cov2 = cov_all[...].reshape(samples, LANES)
    cov_t[...] = jnp.transpose(cov2.astype(F32)).astype(BF16)
    lhs[genes : genes + terms] = cov_t[0:terms]
    gram_wide = gram_of(cov2, cov_t[...])
    small[0] = gram_wide
    inverse = invert(gram_wide)
    eye = jnp.where(lane == row, 1.0, 0.0)[:, 0:covs]
    inverse = inverse + exact_dot(inverse, eye - exact_dot(gram_wide[:, 0:covs], inverse))
    small[1, :, 0:covs] = inverse
    while now() <= min(last, sent_at + far):
        next_tick()

    for k in range(chips):
        block = kept[k]
        fitted = dot(cov_all[k].reshape(2 * rows, LANES), thrice(block[2 * rows :]))
        pheno_all[pl.ds(k * 2 * rows, 2 * rows)] = block[0 : 2 * rows].astype(F32) + fitted
    cov_pheno = jnp.zeros((terms, pad), F32)
    for part in split3(pheno_all[...]):
        cov_pheno = cov_pheno + dot(cov_t[0:terms], part)
    beta = exact_dot(inverse, three_rows(cov_pheno))
    fit = jnp.zeros((samples, pad), F32)
    cov2 = cov_all[...].reshape(samples, LANES)
    for part in split3(beta):
        fit = fit + dot(cov2, thrice(part))
    resid = jnp.transpose(pheno_all[...] - fit)[0:own_genes]
    sumsq = jnp.sum(resid * resid, axis=1, keepdims=True)
    scale = 1.0 / (jnp.sqrt(F32(samples)) * jnp.sqrt(sumsq / samples + 0.1))
    resid_bf = resid.astype(BF16)
    fix = three_lanes(dot(resid_bf, cov2))
    fix_lane = lax.broadcasted_iota(jnp.int32, fix.shape, 1)
    mine_rows = pl.ds(pl.multiple_of(c * own_genes, 16), own_genes)
    lhs[mine_rows] = resid_bf
    lhs_fix[mine_rows] = jnp.where(fix_lane < covs, -fix, 0.0).astype(BF16)
    gene_scale[mine_rows] = jnp.broadcast_to(scale, (own_genes, LANES))
    next_tick()
    pair_rows = [
        pair(3 + k, ref.at[mine_rows], ref.at[mine_rows])
        for k, ref in enumerate((lhs, lhs_fix, gene_scale))
    ]
    for copy in pair_rows:
        copy.start()
    next_tick()
    for copy in pair_rows:
        copy.wait_recv()

    cut = far * 3 // 4 // 4 * 4
    low, high = cut * 2 * rows, (chips - cut) * 2 * rows

    def part(first, final, p):
        dose = dose_all[p, first:final].reshape((final - first) * 2 * rows, width)
        real = dose.astype(F32)
        return (
            dot(lhs[:, first * 2 * rows : final * 2 * rows], dose),
            jnp.sum(real * real, axis=0, keepdims=True),
        )

    def near_part(p):
        if cut:
            before, after = part(0, cut, p), part(chips - cut, chips, p)
            partial[p] = before[0] + after[0]
            partial_sq[p, 0:1] = before[1] + after[1]
        else:
            partial[p] = jnp.zeros(partial.shape[1:], F32)
            partial_sq[p] = jnp.zeros(partial_sq.shape[1:], F32)

    def far_part(p):
        both, dose_sq = part(cut, chips - cut, p)
        both = both + partial[p]
        partial[p, 0:genes] = both[0:genes]
        place = pl.ds(pl.multiple_of(p * width, LANES), width)
        cov_dose_all[:, place] = three_rows(both[genes:])
        dose_sq_all[0:1, place] = dose_sq + partial_sq[p, 0:1]

    def solve_pieces(begin, end):
        span = slice(begin * width, end * width)
        cov_dose = cov_dose_all[:, span]
        beta = exact_dot(small[1, :, 0:covs], cov_dose)
        back = exact_dot(small[0, :, 0:covs], beta)
        dose_sumsq = dose_sq_all[0:1, span] - jnp.sum(
            beta * (2.0 * cov_dose - back), axis=0, keepdims=True
        )
        dose_sq_all[0:1, span] = 1.0 / jnp.sqrt(dose_sumsq / samples + 0.1)
        beta_all[:, span] = beta.astype(BF16)

    def score(p):
        place = pl.ds(pl.multiple_of(p * width, LANES), width)
        dose_scale = dose_sq_all[0:1, place]
        blank = jnp.zeros((LANES - covs, width), BF16)
        cross = partial[p, 0:genes] + dot(
            lhs_fix[...], jnp.concatenate([beta_all[:, place], blank], axis=0)
        )
        scale = gene_scale[...]
        chi_sum, hit_sum = chi_acc[0:genes], hit_acc[0:genes]
        for n in range(width // LANES):
            span = slice(n * LANES, (n + 1) * LANES)
            zscore = cross[:, span] * dose_scale[:, span] * scale
            chi = zscore * zscore
            chi_sum = chi_sum + chi
            hit_sum = hit_sum + 1.0 / (1.0 + jnp.exp(8.0 - 2.0 * chi))
        chi_acc[0:genes] = chi_sum
        hit_acc[0:genes] = hit_sum

    def finish(begin, end):
        over(far_part, begin, end)
        if end > begin:
            solve_pieces(begin, end)
        over(score, begin, end)

    def over(work, begin, end):
        lax.fori_loop(begin, end, lambda p, _: (work(p), 0)[1], 0)

    early = sum(tick_of(p) + far < now() for p in range(PIECES))
    over(near_part, 0, early)
    next_tick()
    finish(0, early)
    next_tick()
    while pending and now() <= last - far // 4 + 1:
        next_tick()
    over(near_part, early, PIECES)
    while pending:
        next_tick()
    finish(early, PIECES)

    mine[...] = jnp.zeros_like(mine)
    mine[0:1] = jnp.sum(jnp.transpose(chi_acc[...]), axis=0, keepdims=True)
    mine[1:2] = jnp.sum(jnp.transpose(hit_acc[...]), axis=0, keepdims=True)
    pair_sums = pair(6, mine, theirs)
    pair_sums.start()
    for p in range(PIECES):
        swap(p).wait_send()
        for d in (CW, CCW):
            for step in range(hops(d, p)):
                ring(d, p, step).wait_send()
    for d in (CW, CCW):
        for step in range(reach[d]):
            ring_cov(d, step).wait_send()
            ring_pheno(d, step).wait_send()
    for copy in (pair_tile, pair_raw, pair_cov, *pair_rows):
        copy.wait_send()
    pair_sums.wait()
    total = mine[...] + theirs[...]
    total = jnp.where(c == 0, total, pltpu.roll(total, total.shape[1] - own_genes, 1))
    chi_ref[...] = total[0:1, 0:own_genes] / variants
    hit_ref[...] = 20.0 / variants * total[1:2, 0:own_genes]


def local(dosage, covars, phenotypes):
    devices = lax.axis_size("tile")
    chips = devices // 2
    rows, variants = dosage.shape
    covs = covars.shape[1]
    genes = phenotypes.shape[1] // chips
    own_genes = genes // 2
    pad = -(-own_genes // LANES) * LANES
    wide = -(-genes // LANES) * LANES
    sent = 2 * rows + covs
    samples = rows * devices
    width = variants // 2 // PIECES
    far = chips // 2
    near = chips - 1 - far
    dma = pltpu.SemaphoreType.DMA
    vmem = pltpu.VMEM
    scratch = [
        vmem(dosage.shape, BF16),
        vmem(covars.shape, F32),
        vmem(phenotypes.shape, F32),
        vmem((PIECES, chips, 2, rows, width), BF16),
        vmem((chips, 2, rows, LANES), BF16),
        vmem((samples, pad), F32),
        vmem((2, rows, chips * pad), F32),
        vmem((2, rows, chips * pad), F32),
        vmem((chips, sent, pad), BF16),
        vmem((far * (far + 1) // 2, sent, pad), BF16),
        vmem((near * (near + 1) // 2, sent, pad), BF16),
        vmem((chips, sent, pad), BF16),
        vmem((rows, LANES), F32),
        vmem((2, rows, LANES), BF16),
        vmem((LANES, samples), BF16),
        vmem((genes + 3 * covs, samples), BF16),
        vmem((genes, LANES), BF16),
        vmem((2, covs, LANES), F32),
        vmem((genes, LANES), F32),
        vmem((PIECES, genes + 3 * covs, width), F32),
        vmem((PIECES, 8, width), F32),
        vmem((covs, PIECES * width), F32),
        vmem((8, PIECES * width), F32),
        vmem((covs, PIECES * width), BF16),
        vmem((wide, LANES), F32),
        vmem((wide, LANES), F32),
        vmem((8, wide), F32),
        vmem((8, wide), F32),
        dma((3,)),
        dma((PIECES,)),
        dma((PIECES,)),
        dma((PIECES,)),
        dma(()),
        dma((2, PIECES, far)),
        dma((2, PIECES, far)),
        dma((2, far)),
        dma((2, far)),
        dma((2, far)),
        dma((2, far)),
        dma((7,)),
        dma((7,)),
    ]
    whole = pl.BlockSpec(memory_space=pltpu.VMEM)
    chi, hit = pl.pallas_call(
        functools.partial(kernel, chips, genes),
        out_shape=[jax.ShapeDtypeStruct((1, own_genes), F32)] * 2,
        in_specs=[pl.BlockSpec(memory_space=pltpu.HBM)] * 3,
        out_specs=[whole] * 2,
        scratch_shapes=scratch,
        compiler_params=pltpu.CompilerParams(
            collective_id=0, has_side_effects=True, vmem_limit_bytes=48 * 2**20
        ),
    )(dosage, covars, phenotypes)
    return chi.reshape(own_genes), hit.reshape(own_genes)


def solution(mesh):
    rows = P(("cohort", "tile"), None)
    return jax.shard_map(
        local,
        mesh=mesh,
        in_specs=(rows, rows, rows),
        out_specs=(P(("cohort", "tile")), P(("cohort", "tile"))),
        check_vma=False,
    )
```

```python
import functools

import jax
import jax.numpy as jnp
from jax import lax
from jax.experimental import pallas as pl
from jax.experimental.pallas import tpu as pltpu
from jax.sharding import PartitionSpec as P

MESH = pl.DeviceIdType.MESH
LANES = 128
PIECES = 8
START = (0, 0, 0, 9, 9, 9, 9, 9)
PHENO_TICK = 1
CW, CCW = 0, 1
F32, BF16 = jnp.float32, jnp.bfloat16


def split3(x):
    hi = x.astype(BF16)
    rest = x - hi.astype(F32)
    mid = rest.astype(BF16)
    lo = (rest - mid.astype(F32)).astype(BF16)
    return hi, mid, lo


def exact_dot(a, b):
    return jnp.dot(a, b, precision=lax.Precision.HIGHEST, preferred_element_type=F32)


def dot(a, b):
    return jnp.dot(a, b, preferred_element_type=F32)


def kernel(
    chips,
    genes,
    dose_hbm,
    cov_hbm,
    pheno_hbm,
    chi_ref,
    hit_ref,
    dose_ref,
    cov_ref,
    pheno_ref,
    dose_all,
    cov_all,
    pheno_all,
    stage,
    chip_raw,
    out_box,
    cw_box,
    ccw_box,
    kept,
    cov_tile,
    chip_tile,
    cov_t,
    lhs,
    lhs_fix,
    small,
    gene_scale,
    partial,
    partial_sq,
    cov_dose_all,
    dose_sq_all,
    beta_all,
    chi_acc,
    hit_acc,
    mine,
    theirs,
    load_sem,
    swap_send,
    swap_recv,
    own_sem,
    raw_sem,
    ring_send,
    ring_recv,
    ph_send,
    ph_recv,
    cv_send,
    cv_recv,
    pair_send,
    pair_recv,
):
    rows, variants = dose_ref.shape
    covs = cov_ref.shape[1]
    half = variants // 2
    width = half // PIECES
    own_genes = genes // 2
    pad = kept.shape[2]
    samples = rows * 2 * chips
    far = chips // 2
    near = chips - 1 - far

    me = lax.axis_index("tile")
    z, c = me // 2, lax.rem(me, 2)
    other = 1 - c
    partner = 2 * z + other
    right = 2 * lax.rem(z + 1, chips) + c
    left = 2 * lax.rem(z + chips - 1, chips) + c
    towards = (right, left)

    def slot(direction, step):
        return (chips - step) % chips if direction == CW else step

    def hops(direction, piece):
        return far if (direction == CW) == (piece == 0) else near

    loads = [
        pltpu.make_async_copy(src, dst, load_sem.at[k])
        for k, (src, dst) in enumerate(
            ((dose_hbm, dose_ref), (cov_hbm, cov_ref), (pheno_hbm, pheno_ref))
        )
    ]
    for copy in loads:
        copy.start()
    barrier = pltpu.get_barrier_semaphore()
    for peer in (partner, right, left):
        pl.semaphore_signal(barrier, inc=1, device_id={"tile": peer}, device_id_type=MESH)
    pl.semaphore_wait(barrier, 3)
    loads[0].wait()

    def swap(p):
        cols = pl.ds(pl.multiple_of(other * half + p * width, LANES), width)
        return pltpu.make_async_remote_copy(
            src_ref=dose_ref.at[:, cols],
            dst_ref=dose_all.at[p, 0, c],
            send_sem=swap_send.at[p],
            recv_sem=swap_recv.at[p],
            device_id={"tile": partner},
            device_id_type=MESH,
        )

    def own(p):
        cols = pl.ds(pl.multiple_of(c * half + p * width, LANES), width)
        return pltpu.make_async_copy(dose_ref.at[:, cols], dose_all.at[p, 0, c], own_sem.at[p])

    def ring(d, p, step):
        return pltpu.make_async_remote_copy(
            src_ref=dose_all.at[p, slot(d, step)],
            dst_ref=dose_all.at[p, slot(d, step + 1)],
            send_sem=ring_send.at[d, p, step],
            recv_sem=ring_recv.at[d, p, step],
            device_id={"tile": towards[d]},
            device_id_type=MESH,
        )

    def ring_cov(d, step):
        return pltpu.make_async_remote_copy(
            src_ref=cov_all.at[slot(d, step), c],
            dst_ref=cov_all.at[slot(d, step + 1), c],
            send_sem=cv_send.at[d, step],
            recv_sem=cv_recv.at[d, step],
            device_id={"tile": towards[d]},
            device_id_type=MESH,
        )

    reach = (far, near)
    boxes = (cw_box, ccw_box)

    def box_start(d, step):
        return sum(reach[d] - k for k in range(step))

    def ring_pheno(d, step):
        count = reach[d] - step
        if step == 0:
            src = out_box.at[pl.ds(1, far)] if d == CW else out_box.at[pl.ds(far + 1, near)]
        else:
            first = box_start(d, step - 1) + (1 if d == CW else 0)
            src = boxes[d].at[pl.ds(first, count)]
        return pltpu.make_async_remote_copy(
            src_ref=src,
            dst_ref=boxes[d].at[pl.ds(box_start(d, step), count)],
            send_sem=ph_send.at[d, step],
            recv_sem=ph_recv.at[d, step],
            device_id={"tile": towards[d]},
            device_id_type=MESH,
        )

    def keep_pheno(d, step):
        at = box_start(d, step) + (0 if d == CW else reach[d] - step - 1)
        kept[slot(d, step + 1)] = boxes[d][at]

    for p in range(PIECES):
        swap(p).start()
        own(p).start()

    def launch(pieces):
        for p in pieces:
            own(p).wait()
            swap(p).wait_recv()
            for d in (CW, CCW):
                ring(d, p, 0).start()

    def tick_of(p):
        return START[p] * far // 16

    launch([p for p in range(PIECES) if tick_of(p) == 0])

    loads[1].wait()
    cov_tile[...] = jnp.zeros_like(cov_tile)
    cov_tile[:, 0:covs] = cov_ref[...]
    hi, mid, lo = split3(cov_tile[...])
    packed = (
        hi.astype(F32)
        + pltpu.roll(mid.astype(F32), covs, 1)
        + pltpu.roll(lo.astype(F32), 2 * covs, 1)
    )
    cov_all[0, c] = packed.astype(BF16)
    chip_tile[c] = packed.astype(BF16)

    loads[2].wait()
    for j in range(chips):
        place = pl.ds(pl.multiple_of(lax.rem(j - z + chips, chips) * pad, LANES), pad)
        for h in range(2):
            begin = genes * j + own_genes * h
            base = begin // LANES * LANES
            wide = min(pad + LANES, pheno_ref.shape[1] - base)
            block = pheno_ref[:, base : base + wide]
            if begin > base:
                block = pltpu.roll(block, wide - (begin - base), 1)
            stage[h, :, place] = block[:, :pad]

    def pair(slot, src, dst):
        return pltpu.make_async_remote_copy(
            src_ref=src,
            dst_ref=dst,
            send_sem=pair_send.at[slot],
            recv_sem=pair_recv.at[slot],
            device_id={"tile": partner},
            device_id_type=MESH,
        )

    pair_tile = pair(0, chip_tile.at[c], chip_tile.at[c])
    pair_raw = pair(1, stage.at[other], chip_raw.at[c])
    own_raw = pltpu.make_async_copy(stage.at[c], chip_raw.at[c], raw_sem)
    pair_tile.start()
    pair_raw.start()
    own_raw.start()
    for d in (CW, CCW):
        ring_cov(d, 0).start()
    chi_acc[...] = jnp.zeros_like(chi_acc)
    hit_acc[...] = jnp.zeros_like(hit_acc)

    lane = lax.broadcasted_iota(jnp.int32, (covs, LANES), 1)
    row = lax.broadcasted_iota(jnp.int32, (covs, LANES), 0)
    terms = 3 * covs

    def three_rows(x):
        return x[0:covs] + x[covs : 2 * covs] + x[2 * covs : terms]

    def three_lanes(x):
        return x + pltpu.roll(x, LANES - covs, 1) + pltpu.roll(x, LANES - 2 * covs, 1)

    def gram_of(x, x_t):
        return jnp.where(lane < covs, three_lanes(three_rows(dot(x_t, x))), 0.0)

    def eliminate(k, a):
        column = jnp.sum(jnp.where(lane == k, a, 0.0), axis=1, keepdims=True)
        pivot_row = jnp.sum(jnp.where(row == k, a, 0.0), axis=0, keepdims=True)
        pivot = jnp.sum(jnp.where(lane[0:1] == k, pivot_row, 0.0), axis=1, keepdims=True)
        pivot_row = pivot_row / pivot
        return jnp.where(row == k, pivot_row, a - column * pivot_row)

    def invert(wide_gram):
        unit = jnp.where(lane == row + covs, 1.0, 0.0)
        solved = lax.fori_loop(0, covs, eliminate, wide_gram + unit)
        return pltpu.roll(solved, LANES - covs, 1)[:, 0:covs]

    def thrice(x):
        blank = jnp.zeros((LANES - terms, x.shape[1]), BF16)
        return jnp.concatenate([x, x, x, blank], axis=0)

    def prepare_pheno():
        pair_tile.wait_recv()
        chip_cov = chip_tile[...].reshape(2 * rows, LANES)
        chip_cov_t = jnp.transpose(chip_cov.astype(F32))
        chip_gram = gram_of(chip_cov, chip_cov_t.astype(BF16))
        ridge = jnp.where(lane == row, chip_gram * 1e-4 + 1e-6, 0.0)
        solve = exact_dot(invert(chip_gram + ridge), three_rows(chip_cov_t))
        solve_hi = solve.astype(BF16)
        solve_lo = (solve - solve_hi.astype(F32)).astype(BF16)
        solver = jnp.concatenate([solve_hi, solve_lo], axis=0)
        next_tick()
        own_raw.wait()
        pair_raw.wait_recv()
        group = 8 * pad

        def fit_group(g, carry):
            place = pl.ds(pl.multiple_of(g * group, LANES), group)
            raw = chip_raw[:, :, place].reshape(2 * rows, group)
            both = dot(solver, raw.astype(BF16))
            beta = (both[0:covs] + both[covs : 2 * covs]).astype(BF16)
            left_over = (raw - dot(chip_cov, thrice(beta))).astype(BF16)
            for k in range(8):
                cut = slice(k * pad, (k + 1) * pad)
                out_box[g * 8 + k, 0 : 2 * rows] = left_over[:, cut]
                out_box[g * 8 + k, 2 * rows : 2 * rows + covs] = beta[:, cut]
            return carry

        half_groups = chips // 16
        lax.fori_loop(0, half_groups, fit_group, 0)
        next_tick()
        lax.fori_loop(half_groups, chips // 8, fit_group, 0)

    def launch_pheno():
        for d in (CW, CCW):
            ring_pheno(d, 0).start()
        kept[0] = out_box[0]

    def forward(p, step):
        for d in (CW, CCW):
            if 0 <= step - 1 < hops(d, p):
                ring(d, p, step - 1).wait_recv()
            if 0 < step < hops(d, p):
                ring(d, p, step).start()

    sent_at = 2 + PHENO_TICK

    def tick(t, then=None):
        launch([p for p in range(PIECES) if t > 0 and tick_of(p) == t])
        for d in (CW, CCW):
            if 0 < t <= reach[d]:
                ring_cov(d, t - 1).wait_recv()
            if 0 < t < reach[d]:
                ring_cov(d, t).start()
        for p in sorted(range(PIECES), key=tick_of):
            if 0 < t - tick_of(p) <= far:
                forward(p, t - tick_of(p))
                if then and t - tick_of(p) == far:
                    then(p)
        step = t - sent_at
        for d in (CW, CCW):
            if 0 < step <= reach[d]:
                ring_pheno(d, step - 1).wait_recv()
            if 0 < step < reach[d]:
                ring_pheno(d, step).start()
            if 0 < step <= reach[d]:
                keep_pheno(d, step - 1)

    last = max([tick_of(p) for p in range(PIECES)] + [sent_at + 1]) + far
    pending = list(range(1, last + 1))

    def now():
        return pending[0] if pending else last + 1

    def next_tick(then=None):
        if pending:
            tick(pending.pop(0), then)

    for _ in range(sent_at - 2):
        next_tick()
    prepare_pheno()
    launch_pheno()
    while now() <= far:
        next_tick()

    pair_cov = pair(2, cov_all.at[:, c], cov_all.at[:, c])
    pair_cov.start()

    next_tick()
    pair_cov.wait_recv()
    cov2 = cov_all[...].reshape(samples, LANES)
    cov_t[...] = jnp.transpose(cov2.astype(F32)).astype(BF16)
    lhs[genes : genes + terms] = cov_t[0:terms]
    gram_wide = gram_of(cov2, cov_t[...])
    small[0] = gram_wide
    inverse = invert(gram_wide)
    eye = jnp.where(lane == row, 1.0, 0.0)[:, 0:covs]
    inverse = inverse + exact_dot(inverse, eye - exact_dot(gram_wide[:, 0:covs], inverse))
    small[1, :, 0:covs] = inverse
    while now() <= min(last, sent_at + far):
        next_tick()

    for k in range(chips):
        block = kept[k]
        fitted = dot(cov_all[k].reshape(2 * rows, LANES), thrice(block[2 * rows :]))
        pheno_all[pl.ds(k * 2 * rows, 2 * rows)] = block[0 : 2 * rows].astype(F32) + fitted
    cov_pheno = jnp.zeros((terms, pad), F32)
    for part in split3(pheno_all[...]):
        cov_pheno = cov_pheno + dot(cov_t[0:terms], part)
    beta = exact_dot(inverse, three_rows(cov_pheno))
    fit = jnp.zeros((samples, pad), F32)
    cov2 = cov_all[...].reshape(samples, LANES)
    for part in split3(beta):
        fit = fit + dot(cov2, thrice(part))
    resid = jnp.transpose(pheno_all[...] - fit)[0:own_genes]
    sumsq = jnp.sum(resid * resid, axis=1, keepdims=True)
    scale = 1.0 / (jnp.sqrt(F32(samples)) * jnp.sqrt(sumsq / samples + 0.1))
    resid_bf = resid.astype(BF16)
    fix = three_lanes(dot(resid_bf, cov2))
    fix_lane = lax.broadcasted_iota(jnp.int32, fix.shape, 1)
    mine_rows = pl.ds(pl.multiple_of(c * own_genes, 16), own_genes)
    lhs[mine_rows] = resid_bf
    lhs_fix[mine_rows] = jnp.where(fix_lane < covs, -fix, 0.0).astype(BF16)
    gene_scale[mine_rows] = jnp.broadcast_to(scale, (own_genes, LANES))
    next_tick()
    pair_rows = [
        pair(3 + k, ref.at[mine_rows], ref.at[mine_rows])
        for k, ref in enumerate((lhs, lhs_fix, gene_scale))
    ]
    for copy in pair_rows:
        copy.start()
    next_tick()
    for copy in pair_rows:
        copy.wait_recv()

    cut = far * 3 // 4 // 4 * 4
    low, high = cut * 2 * rows, (chips - cut) * 2 * rows

    def part(first, final, p):
        dose = dose_all[p, first:final].reshape((final - first) * 2 * rows, width)
        real = dose.astype(F32)
        return (
            dot(lhs[:, first * 2 * rows : final * 2 * rows], dose),
            jnp.sum(real * real, axis=0, keepdims=True),
        )

    def near_part(p):
        if cut:
            before, after = part(0, cut, p), part(chips - cut, chips, p)
            partial[p] = before[0] + after[0]
            partial_sq[p, 0:1] = before[1] + after[1]
        else:
            partial[p] = jnp.zeros(partial.shape[1:], F32)
            partial_sq[p] = jnp.zeros(partial_sq.shape[1:], F32)

    def far_part(p):
        both, dose_sq = part(cut, chips - cut, p)
        both = both + partial[p]
        partial[p, 0:genes] = both[0:genes]
        place = pl.ds(pl.multiple_of(p * width, LANES), width)
        cov_dose_all[:, place] = three_rows(both[genes:])
        dose_sq_all[0:1, place] = dose_sq + partial_sq[p, 0:1]

    def solve_pieces(begin, end):
        span = slice(begin * width, end * width)
        cov_dose = cov_dose_all[:, span]
        beta = exact_dot(small[1, :, 0:covs], cov_dose)
        back = exact_dot(small[0, :, 0:covs], beta)
        dose_sumsq = dose_sq_all[0:1, span] - jnp.sum(
            beta * (2.0 * cov_dose - back), axis=0, keepdims=True
        )
        dose_sq_all[0:1, span] = 1.0 / jnp.sqrt(dose_sumsq / samples + 0.1)
        beta_all[:, span] = beta.astype(BF16)

    def score(p):
        place = pl.ds(pl.multiple_of(p * width, LANES), width)
        dose_scale = dose_sq_all[0:1, place]
        blank = jnp.zeros((LANES - covs, width), BF16)
        cross = partial[p, 0:genes] + dot(
            lhs_fix[...], jnp.concatenate([beta_all[:, place], blank], axis=0)
        )
        scale = gene_scale[...]
        chi_sum, hit_sum = chi_acc[0:genes], hit_acc[0:genes]
        for n in range(width // LANES):
            span = slice(n * LANES, (n + 1) * LANES)
            zscore = cross[:, span] * dose_scale[:, span] * scale
            chi = zscore * zscore
            chi_sum = chi_sum + chi
            hit_sum = hit_sum + 1.0 / (1.0 + jnp.exp(8.0 - 2.0 * chi))
        chi_acc[0:genes] = chi_sum
        hit_acc[0:genes] = hit_sum

    def finish(begin, end):
        if end > begin:
            solve_pieces(begin, end)
        over(score, begin, end)

    def over(work, begin, end):
        lax.fori_loop(begin, end, lambda p, _: (work(p), 0)[1], 0)

    early = sum(tick_of(p) + far < now() for p in range(PIECES))
    over(near_part, 0, early)
    next_tick()
    over(far_part, 0, early)
    finish(0, early)
    next_tick()
    while pending and now() <= last - far // 4 + 1:
        next_tick()
    over(near_part, early, PIECES)
    landed = []

    def land(p):
        if p >= early:
            far_part(p)
            landed.append(p)

    while pending:
        next_tick(land)
    for p in range(early, PIECES):
        if p not in landed:
            far_part(p)
    finish(early, PIECES)

    mine[...] = jnp.zeros_like(mine)
    mine[0:1] = jnp.sum(jnp.transpose(chi_acc[...]), axis=0, keepdims=True)
    mine[1:2] = jnp.sum(jnp.transpose(hit_acc[...]), axis=0, keepdims=True)
    pair_sums = pair(6, mine, theirs)
    pair_sums.start()
    for p in range(PIECES):
        swap(p).wait_send()
        for d in (CW, CCW):
            for step in range(hops(d, p)):
                ring(d, p, step).wait_send()
    for d in (CW, CCW):
        for step in range(reach[d]):
            ring_cov(d, step).wait_send()
            ring_pheno(d, step).wait_send()
    for copy in (pair_tile, pair_raw, pair_cov, *pair_rows):
        copy.wait_send()
    pair_sums.wait()
    total = mine[...] + theirs[...]
    total = jnp.where(c == 0, total, pltpu.roll(total, total.shape[1] - own_genes, 1))
    chi_ref[...] = total[0:1, 0:own_genes] / variants
    hit_ref[...] = 20.0 / variants * total[1:2, 0:own_genes]


def local(dosage, covars, phenotypes):
    devices = lax.axis_size("tile")
    chips = devices // 2
    rows, variants = dosage.shape
    covs = covars.shape[1]
    genes = phenotypes.shape[1] // chips
    own_genes = genes // 2
    pad = -(-own_genes // LANES) * LANES
    wide = -(-genes // LANES) * LANES
    sent = 2 * rows + covs
    samples = rows * devices
    width = variants // 2 // PIECES
    far = chips // 2
    near = chips - 1 - far
    dma = pltpu.SemaphoreType.DMA
    vmem = pltpu.VMEM
    scratch = [
        vmem(dosage.shape, BF16),
        vmem(covars.shape, F32),
        vmem(phenotypes.shape, F32),
        vmem((PIECES, chips, 2, rows, width), BF16),
        vmem((chips, 2, rows, LANES), BF16),
        vmem((samples, pad), F32),
        vmem((2, rows, chips * pad), F32),
        vmem((2, rows, chips * pad), F32),
        vmem((chips, sent, pad), BF16),
        vmem((far * (far + 1) // 2, sent, pad), BF16),
        vmem((near * (near + 1) // 2, sent, pad), BF16),
        vmem((chips, sent, pad), BF16),
        vmem((rows, LANES), F32),
        vmem((2, rows, LANES), BF16),
        vmem((LANES, samples), BF16),
        vmem((genes + 3 * covs, samples), BF16),
        vmem((genes, LANES), BF16),
        vmem((2, covs, LANES), F32),
        vmem((genes, LANES), F32),
        vmem((PIECES, genes + 3 * covs, width), F32),
        vmem((PIECES, 8, width), F32),
        vmem((covs, PIECES * width), F32),
        vmem((8, PIECES * width), F32),
        vmem((covs, PIECES * width), BF16),
        vmem((wide, LANES), F32),
        vmem((wide, LANES), F32),
        vmem((8, wide), F32),
        vmem((8, wide), F32),
        dma((3,)),
        dma((PIECES,)),
        dma((PIECES,)),
        dma((PIECES,)),
        dma(()),
        dma((2, PIECES, far)),
        dma((2, PIECES, far)),
        dma((2, far)),
        dma((2, far)),
        dma((2, far)),
        dma((2, far)),
        dma((7,)),
        dma((7,)),
    ]
    whole = pl.BlockSpec(memory_space=pltpu.VMEM)
    chi, hit = pl.pallas_call(
        functools.partial(kernel, chips, genes),
        out_shape=[jax.ShapeDtypeStruct((1, own_genes), F32)] * 2,
        in_specs=[pl.BlockSpec(memory_space=pltpu.HBM)] * 3,
        out_specs=[whole] * 2,
        scratch_shapes=scratch,
        compiler_params=pltpu.CompilerParams(
            collective_id=0, has_side_effects=True, vmem_limit_bytes=48 * 2**20
        ),
    )(dosage, covars, phenotypes)
    return chi.reshape(own_genes), hit.reshape(own_genes)


def solution(mesh):
    rows = P(("cohort", "tile"), None)
    return jax.shard_map(
        local,
        mesh=mesh,
        in_specs=(rows, rows, rows),
        out_specs=(P(("cohort", "tile")), P(("cohort", "tile"))),
        check_vma=False,
    )
```

```python
import functools

import jax
import jax.numpy as jnp
from jax import lax
from jax.experimental import pallas as pl
from jax.experimental.pallas import tpu as pltpu
from jax.sharding import PartitionSpec as P

MESH = pl.DeviceIdType.MESH
LANES = 128
PIECES = 8
START = (0, 0, 0, 9, 9, 9, 9, 9)
PHENO_TICK = 1
CW, CCW = 0, 1
F32, BF16 = jnp.float32, jnp.bfloat16


def split3(x):
    hi = x.astype(BF16)
    rest = x - hi.astype(F32)
    mid = rest.astype(BF16)
    lo = (rest - mid.astype(F32)).astype(BF16)
    return hi, mid, lo


def exact_dot(a, b):
    return jnp.dot(a, b, precision=lax.Precision.HIGHEST, preferred_element_type=F32)


def dot(a, b):
    return jnp.dot(a, b, preferred_element_type=F32)


def kernel(
    chips,
    genes,
    dose_hbm,
    cov_hbm,
    pheno_hbm,
    chi_ref,
    hit_ref,
    dose_ref,
    cov_ref,
    pheno_ref,
    dose_all,
    cov_all,
    pheno_all,
    stage,
    chip_raw,
    out_box,
    cw_box,
    ccw_box,
    kept,
    cov_tile,
    chip_tile,
    cov_t,
    lhs,
    lhs_fix,
    small,
    gene_scale,
    partial,
    partial_sq,
    cov_dose_all,
    dose_sq_all,
    beta_all,
    chi_acc,
    hit_acc,
    mine,
    theirs,
    load_sem,
    swap_send,
    swap_recv,
    own_sem,
    raw_sem,
    ring_send,
    ring_recv,
    ph_send,
    ph_recv,
    cv_send,
    cv_recv,
    pair_send,
    pair_recv,
):
    rows, variants = dose_ref.shape
    covs = cov_ref.shape[1]
    half = variants // 2
    width = half // PIECES
    own_genes = genes // 2
    pad = kept.shape[2]
    samples = rows * 2 * chips
    far = chips // 2
    near = chips - 1 - far

    me = lax.axis_index("tile")
    z, c = me // 2, lax.rem(me, 2)
    other = 1 - c
    partner = 2 * z + other
    right = 2 * lax.rem(z + 1, chips) + c
    left = 2 * lax.rem(z + chips - 1, chips) + c
    towards = (right, left)

    def slot(direction, step):
        return (chips - step) % chips if direction == CW else step

    def hops(direction, piece):
        return far if (direction == CW) == (piece == 0) else near

    loads = [
        pltpu.make_async_copy(src, dst, load_sem.at[k])
        for k, (src, dst) in enumerate(
            ((dose_hbm, dose_ref), (cov_hbm, cov_ref), (pheno_hbm, pheno_ref))
        )
    ]
    for copy in loads:
        copy.start()
    barrier = pltpu.get_barrier_semaphore()
    for peer in (partner, right, left):
        pl.semaphore_signal(barrier, inc=1, device_id={"tile": peer}, device_id_type=MESH)
    pl.semaphore_wait(barrier, 3)
    loads[0].wait()

    def swap(p):
        cols = pl.ds(pl.multiple_of(other * half + p * width, LANES), width)
        return pltpu.make_async_remote_copy(
            src_ref=dose_ref.at[:, cols],
            dst_ref=dose_all.at[p, 0, c],
            send_sem=swap_send.at[p],
            recv_sem=swap_recv.at[p],
            device_id={"tile": partner},
            device_id_type=MESH,
        )

    def own(p):
        cols = pl.ds(pl.multiple_of(c * half + p * width, LANES), width)
        return pltpu.make_async_copy(dose_ref.at[:, cols], dose_all.at[p, 0, c], own_sem.at[p])

    def ring(d, p, step):
        return pltpu.make_async_remote_copy(
            src_ref=dose_all.at[p, slot(d, step)],
            dst_ref=dose_all.at[p, slot(d, step + 1)],
            send_sem=ring_send.at[d, p, step],
            recv_sem=ring_recv.at[d, p, step],
            device_id={"tile": towards[d]},
            device_id_type=MESH,
        )

    def ring_cov(d, step):
        return pltpu.make_async_remote_copy(
            src_ref=cov_all.at[slot(d, step), c],
            dst_ref=cov_all.at[slot(d, step + 1), c],
            send_sem=cv_send.at[d, step],
            recv_sem=cv_recv.at[d, step],
            device_id={"tile": towards[d]},
            device_id_type=MESH,
        )

    reach = (far, near)
    boxes = (cw_box, ccw_box)

    def box_start(d, step):
        return sum(reach[d] - k for k in range(step))

    def ring_pheno(d, step):
        count = reach[d] - step
        if step == 0:
            src = out_box.at[pl.ds(1, far)] if d == CW else out_box.at[pl.ds(far + 1, near)]
        else:
            first = box_start(d, step - 1) + (1 if d == CW else 0)
            src = boxes[d].at[pl.ds(first, count)]
        return pltpu.make_async_remote_copy(
            src_ref=src,
            dst_ref=boxes[d].at[pl.ds(box_start(d, step), count)],
            send_sem=ph_send.at[d, step],
            recv_sem=ph_recv.at[d, step],
            device_id={"tile": towards[d]},
            device_id_type=MESH,
        )

    def keep_pheno(d, step):
        at = box_start(d, step) + (0 if d == CW else reach[d] - step - 1)
        kept[slot(d, step + 1)] = boxes[d][at]

    for p in range(PIECES):
        swap(p).start()
        own(p).start()

    def launch(pieces):
        for p in pieces:
            own(p).wait()
            swap(p).wait_recv()
            for d in (CW, CCW):
                ring(d, p, 0).start()

    def tick_of(p):
        return START[p] * far // 16

    launch([p for p in range(PIECES) if tick_of(p) == 0])

    loads[1].wait()
    cov_tile[...] = jnp.zeros_like(cov_tile)
    cov_tile[:, 0:covs] = cov_ref[...]
    hi, mid, lo = split3(cov_tile[...])
    packed = (
        hi.astype(F32)
        + pltpu.roll(mid.astype(F32), covs, 1)
        + pltpu.roll(lo.astype(F32), 2 * covs, 1)
    )
    cov_all[0, c] = packed.astype(BF16)
    chip_tile[c] = packed.astype(BF16)

    loads[2].wait()
    for j in range(chips):
        place = pl.ds(pl.multiple_of(lax.rem(j - z + chips, chips) * pad, LANES), pad)
        for h in range(2):
            begin = genes * j + own_genes * h
            base = begin // LANES * LANES
            wide = min(pad + LANES, pheno_ref.shape[1] - base)
            block = pheno_ref[:, base : base + wide]
            if begin > base:
                block = pltpu.roll(block, wide - (begin - base), 1)
            stage[h, :, place] = block[:, :pad]

    def pair(slot, src, dst):
        return pltpu.make_async_remote_copy(
            src_ref=src,
            dst_ref=dst,
            send_sem=pair_send.at[slot],
            recv_sem=pair_recv.at[slot],
            device_id={"tile": partner},
            device_id_type=MESH,
        )

    pair_tile = pair(0, chip_tile.at[c], chip_tile.at[c])
    pair_raw = pair(1, stage.at[other], chip_raw.at[c])
    own_raw = pltpu.make_async_copy(stage.at[c], chip_raw.at[c], raw_sem)
    pair_tile.start()
    pair_raw.start()
    own_raw.start()
    for d in (CW, CCW):
        ring_cov(d, 0).start()
    chi_acc[...] = jnp.zeros_like(chi_acc)
    hit_acc[...] = jnp.zeros_like(hit_acc)

    lane = lax.broadcasted_iota(jnp.int32, (covs, LANES), 1)
    row = lax.broadcasted_iota(jnp.int32, (covs, LANES), 0)
    terms = 3 * covs

    def three_rows(x):
        return x[0:covs] + x[covs : 2 * covs] + x[2 * covs : terms]

    def three_lanes(x):
        return x + pltpu.roll(x, LANES - covs, 1) + pltpu.roll(x, LANES - 2 * covs, 1)

    def gram_of(x, x_t):
        return jnp.where(lane < covs, three_lanes(three_rows(dot(x_t, x))), 0.0)

    def eliminate(k, a):
        column = jnp.sum(jnp.where(lane == k, a, 0.0), axis=1, keepdims=True)
        pivot_row = jnp.sum(jnp.where(row == k, a, 0.0), axis=0, keepdims=True)
        pivot = jnp.sum(jnp.where(lane[0:1] == k, pivot_row, 0.0), axis=1, keepdims=True)
        pivot_row = pivot_row / pivot
        return jnp.where(row == k, pivot_row, a - column * pivot_row)

    def invert(wide_gram):
        unit = jnp.where(lane == row + covs, 1.0, 0.0)
        solved = lax.fori_loop(0, covs, eliminate, wide_gram + unit)
        return pltpu.roll(solved, LANES - covs, 1)[:, 0:covs]

    def thrice(x):
        blank = jnp.zeros((LANES - terms, x.shape[1]), BF16)
        return jnp.concatenate([x, x, x, blank], axis=0)

    def prepare_pheno():
        pair_tile.wait_recv()
        chip_cov = chip_tile[...].reshape(2 * rows, LANES)
        chip_cov_t = jnp.transpose(chip_cov.astype(F32))
        chip_gram = gram_of(chip_cov, chip_cov_t.astype(BF16))
        ridge = jnp.where(lane == row, chip_gram * 1e-4 + 1e-6, 0.0)
        solve = exact_dot(invert(chip_gram + ridge), three_rows(chip_cov_t))
        solve_hi = solve.astype(BF16)
        solve_lo = (solve - solve_hi.astype(F32)).astype(BF16)
        solver = jnp.concatenate([solve_hi, solve_lo], axis=0)
        next_tick()
        own_raw.wait()
        pair_raw.wait_recv()
        group = 8 * pad

        def fit_group(g, carry):
            place = pl.ds(pl.multiple_of(g * group, LANES), group)
            raw = chip_raw[:, :, place].reshape(2 * rows, group)
            both = dot(solver, raw.astype(BF16))
            beta = (both[0:covs] + both[covs : 2 * covs]).astype(BF16)
            left_over = (raw - dot(chip_cov, thrice(beta))).astype(BF16)
            for k in range(8):
                cut = slice(k * pad, (k + 1) * pad)
                out_box[g * 8 + k, 0 : 2 * rows] = left_over[:, cut]
                out_box[g * 8 + k, 2 * rows : 2 * rows + covs] = beta[:, cut]
            return carry

        half_groups = chips // 16
        lax.fori_loop(0, half_groups, fit_group, 0)
        next_tick()
        lax.fori_loop(half_groups, chips // 8, fit_group, 0)

    def launch_pheno():
        for d in (CW, CCW):
            ring_pheno(d, 0).start()
        kept[0] = out_box[0]

    def forward(p, step):
        for d in (CW, CCW):
            if 0 <= step - 1 < hops(d, p):
                ring(d, p, step - 1).wait_recv()
            if 0 < step < hops(d, p):
                ring(d, p, step).start()

    sent_at = 2 + PHENO_TICK

    def tick(t, then=None):
        launch([p for p in range(PIECES) if t > 0 and tick_of(p) == t])
        for d in (CW, CCW):
            if 0 < t <= reach[d]:
                ring_cov(d, t - 1).wait_recv()
            if 0 < t < reach[d]:
                ring_cov(d, t).start()
        for p in sorted(range(PIECES), key=tick_of):
            if 0 < t - tick_of(p) <= far:
                forward(p, t - tick_of(p))
                if then:
                    then(p, t - tick_of(p))
        step = t - sent_at
        for d in (CW, CCW):
            if 0 < step <= reach[d]:
                ring_pheno(d, step - 1).wait_recv()
            if 0 < step < reach[d]:
                ring_pheno(d, step).start()
            if 0 < step <= reach[d]:
                keep_pheno(d, step - 1)

    last = max([tick_of(p) for p in range(PIECES)] + [sent_at + 1]) + far
    pending = list(range(1, last + 1))

    def now():
        return pending[0] if pending else last + 1

    def next_tick(then=None):
        if pending:
            tick(pending.pop(0), then)

    for _ in range(sent_at - 2):
        next_tick()
    prepare_pheno()
    launch_pheno()
    while now() <= far:
        next_tick()

    pair_cov = pair(2, cov_all.at[:, c], cov_all.at[:, c])
    pair_cov.start()

    next_tick()
    pair_cov.wait_recv()
    cov2 = cov_all[...].reshape(samples, LANES)
    cov_t[...] = jnp.transpose(cov2.astype(F32)).astype(BF16)
    lhs[genes : genes + terms] = cov_t[0:terms]
    gram_wide = gram_of(cov2, cov_t[...])
    small[0] = gram_wide
    inverse = invert(gram_wide)
    eye = jnp.where(lane == row, 1.0, 0.0)[:, 0:covs]
    inverse = inverse + exact_dot(inverse, eye - exact_dot(gram_wide[:, 0:covs], inverse))
    small[1, :, 0:covs] = inverse
    while now() <= min(last, sent_at + far):
        next_tick()

    for k in range(chips):
        block = kept[k]
        fitted = dot(cov_all[k].reshape(2 * rows, LANES), thrice(block[2 * rows :]))
        pheno_all[pl.ds(k * 2 * rows, 2 * rows)] = block[0 : 2 * rows].astype(F32) + fitted
    cov_pheno = jnp.zeros((terms, pad), F32)
    for part in split3(pheno_all[...]):
        cov_pheno = cov_pheno + dot(cov_t[0:terms], part)
    beta = exact_dot(inverse, three_rows(cov_pheno))
    fit = jnp.zeros((samples, pad), F32)
    cov2 = cov_all[...].reshape(samples, LANES)
    for part in split3(beta):
        fit = fit + dot(cov2, thrice(part))
    resid = jnp.transpose(pheno_all[...] - fit)[0:own_genes]
    sumsq = jnp.sum(resid * resid, axis=1, keepdims=True)
    scale = 1.0 / (jnp.sqrt(F32(samples)) * jnp.sqrt(sumsq / samples + 0.1))
    resid_bf = resid.astype(BF16)
    fix = three_lanes(dot(resid_bf, cov2))
    fix_lane = lax.broadcasted_iota(jnp.int32, fix.shape, 1)
    mine_rows = pl.ds(pl.multiple_of(c * own_genes, 16), own_genes)
    lhs[mine_rows] = resid_bf
    lhs_fix[mine_rows] = jnp.where(fix_lane < covs, -fix, 0.0).astype(BF16)
    gene_scale[mine_rows] = jnp.broadcast_to(scale, (own_genes, LANES))
    next_tick()
    pair_rows = [
        pair(3 + k, ref.at[mine_rows], ref.at[mine_rows])
        for k, ref in enumerate((lhs, lhs_fix, gene_scale))
    ]
    for copy in pair_rows:
        copy.start()
    next_tick()
    for copy in pair_rows:
        copy.wait_recv()

    cut = far * 3 // 4 // 4 * 4
    low, high = cut * 2 * rows, (chips - cut) * 2 * rows

    def part(first, final, p):
        dose = dose_all[p, first:final].reshape((final - first) * 2 * rows, width)
        real = dose.astype(F32)
        return (
            dot(lhs[:, first * 2 * rows : final * 2 * rows], dose),
            jnp.sum(real * real, axis=0, keepdims=True),
        )

    def near_part(p):
        if cut:
            before, after = part(0, cut, p), part(chips - cut, chips, p)
            partial[p] = before[0] + after[0]
            partial_sq[p, 0:1] = before[1] + after[1]
        else:
            partial[p] = jnp.zeros(partial.shape[1:], F32)
            partial_sq[p] = jnp.zeros(partial_sq.shape[1:], F32)

    def far_part(p):
        both, dose_sq = part(cut, chips - cut, p)
        both = both + partial[p]
        partial[p, 0:genes] = both[0:genes]
        place = pl.ds(pl.multiple_of(p * width, LANES), width)
        cov_dose_all[:, place] = three_rows(both[genes:])
        dose_sq_all[0:1, place] = dose_sq + partial_sq[p, 0:1]

    def solve_pieces(begin, end):
        span = slice(begin * width, end * width)
        cov_dose = cov_dose_all[:, span]
        beta = exact_dot(small[1, :, 0:covs], cov_dose)
        back = exact_dot(small[0, :, 0:covs], beta)
        dose_sumsq = dose_sq_all[0:1, span] - jnp.sum(
            beta * (2.0 * cov_dose - back), axis=0, keepdims=True
        )
        dose_sq_all[0:1, span] = 1.0 / jnp.sqrt(dose_sumsq / samples + 0.1)
        beta_all[:, span] = beta.astype(BF16)

    def score(p):
        place = pl.ds(pl.multiple_of(p * width, LANES), width)
        dose_scale = dose_sq_all[0:1, place]
        blank = jnp.zeros((LANES - covs, width), BF16)
        cross = partial[p, 0:genes] + dot(
            lhs_fix[...], jnp.concatenate([beta_all[:, place], blank], axis=0)
        )
        scale = gene_scale[...]
        chi_sum, hit_sum = chi_acc[0:genes], hit_acc[0:genes]
        for n in range(width // LANES):
            span = slice(n * LANES, (n + 1) * LANES)
            zscore = cross[:, span] * dose_scale[:, span] * scale
            chi = zscore * zscore
            chi_sum = chi_sum + chi
            hit_sum = hit_sum + 1.0 / (1.0 + jnp.exp(8.0 - 2.0 * chi))
        chi_acc[0:genes] = chi_sum
        hit_acc[0:genes] = hit_sum

    def finish(begin, end):
        if end > begin:
            solve_pieces(begin, end)
        over(score, begin, end)

    def over(work, begin, end):
        lax.fori_loop(begin, end, lambda p, _: (work(p), 0)[1], 0)

    early = sum(tick_of(p) + far < now() for p in range(PIECES))
    over(near_part, 0, early)
    next_tick()
    over(far_part, 0, early)
    finish(0, early)
    next_tick()
    while pending and now() <= last - far // 4 + 1:
        next_tick()
    ready = []

    def prepare(p, step):
        if p >= early and step > cut and p not in ready:
            near_part(p)
            ready.append(p)

    next_tick(prepare)
    for p in range(early, PIECES):
        if p not in ready:
            near_part(p)
    landed = []

    def land(p, step):
        if p >= early and step == far:
            far_part(p)
            landed.append(p)

    while pending:
        next_tick(land)
    for p in range(early, PIECES):
        if p not in landed:
            far_part(p)
    finish(early, PIECES)

    mine[...] = jnp.zeros_like(mine)
    mine[0:1] = jnp.sum(jnp.transpose(chi_acc[...]), axis=0, keepdims=True)
    mine[1:2] = jnp.sum(jnp.transpose(hit_acc[...]), axis=0, keepdims=True)
    pair_sums = pair(6, mine, theirs)
    pair_sums.start()
    for p in range(PIECES):
        swap(p).wait_send()
        for d in (CW, CCW):
            for step in range(hops(d, p)):
                ring(d, p, step).wait_send()
    for d in (CW, CCW):
        for step in range(reach[d]):
            ring_cov(d, step).wait_send()
            ring_pheno(d, step).wait_send()
    for copy in (pair_tile, pair_raw, pair_cov, *pair_rows):
        copy.wait_send()
    pair_sums.wait()
    total = mine[...] + theirs[...]
    total = jnp.where(c == 0, total, pltpu.roll(total, total.shape[1] - own_genes, 1))
    chi_ref[...] = total[0:1, 0:own_genes] / variants
    hit_ref[...] = 20.0 / variants * total[1:2, 0:own_genes]


def local(dosage, covars, phenotypes):
    devices = lax.axis_size("tile")
    chips = devices // 2
    rows, variants = dosage.shape
    covs = covars.shape[1]
    genes = phenotypes.shape[1] // chips
    own_genes = genes // 2
    pad = -(-own_genes // LANES) * LANES
    wide = -(-genes // LANES) * LANES
    sent = 2 * rows + covs
    samples = rows * devices
    width = variants // 2 // PIECES
    far = chips // 2
    near = chips - 1 - far
    dma = pltpu.SemaphoreType.DMA
    vmem = pltpu.VMEM
    scratch = [
        vmem(dosage.shape, BF16),
        vmem(covars.shape, F32),
        vmem(phenotypes.shape, F32),
        vmem((PIECES, chips, 2, rows, width), BF16),
        vmem((chips, 2, rows, LANES), BF16),
        vmem((samples, pad), F32),
        vmem((2, rows, chips * pad), F32),
        vmem((2, rows, chips * pad), F32),
        vmem((chips, sent, pad), BF16),
        vmem((far * (far + 1) // 2, sent, pad), BF16),
        vmem((near * (near + 1) // 2, sent, pad), BF16),
        vmem((chips, sent, pad), BF16),
        vmem((rows, LANES), F32),
        vmem((2, rows, LANES), BF16),
        vmem((LANES, samples), BF16),
        vmem((genes + 3 * covs, samples), BF16),
        vmem((genes, LANES), BF16),
        vmem((2, covs, LANES), F32),
        vmem((genes, LANES), F32),
        vmem((PIECES, genes + 3 * covs, width), F32),
        vmem((PIECES, 8, width), F32),
        vmem((covs, PIECES * width), F32),
        vmem((8, PIECES * width), F32),
        vmem((covs, PIECES * width), BF16),
        vmem((wide, LANES), F32),
        vmem((wide, LANES), F32),
        vmem((8, wide), F32),
        vmem((8, wide), F32),
        dma((3,)),
        dma((PIECES,)),
        dma((PIECES,)),
        dma((PIECES,)),
        dma(()),
        dma((2, PIECES, far)),
        dma((2, PIECES, far)),
        dma((2, far)),
        dma((2, far)),
        dma((2, far)),
        dma((2, far)),
        dma((7,)),
        dma((7,)),
    ]
    whole = pl.BlockSpec(memory_space=pltpu.VMEM)
    chi, hit = pl.pallas_call(
        functools.partial(kernel, chips, genes),
        out_shape=[jax.ShapeDtypeStruct((1, own_genes), F32)] * 2,
        in_specs=[pl.BlockSpec(memory_space=pltpu.HBM)] * 3,
        out_specs=[whole] * 2,
        scratch_shapes=scratch,
        compiler_params=pltpu.CompilerParams(
            collective_id=0, has_side_effects=True, vmem_limit_bytes=48 * 2**20
        ),
    )(dosage, covars, phenotypes)
    return chi.reshape(own_genes), hit.reshape(own_genes)


def solution(mesh):
    rows = P(("cohort", "tile"), None)
    return jax.shard_map(
        local,
        mesh=mesh,
        in_specs=(rows, rows, rows),
        out_specs=(P(("cohort", "tile")), P(("cohort", "tile"))),
        check_vma=False,
    )
```
